1024 devices in a mesh: fsdp: 16 (over x, core), ep: 64 (over z, y).
Axes of the slice: x: 8, y: 8, z: 8, core: 2. Of those that a mesh axis runs over, the one named last changes fastest.
Arguments:
- tokens: bfloat16 [8192, 2048], P(('fsdp', 'ep')), may hold values from -6 to 6
- cotangent: bfloat16 [8192, 2048], P(('fsdp', 'ep')), may hold values from -4 to 4
- routes: int32 [8192, 2], P(('fsdp', 'ep')), may hold values from 0 to 7, as said below
- logits: float32 [8192, 8], P(('fsdp', 'ep')), may hold values from -8 to 8
- w_gate: bfloat16 [2048, 16384], P('fsdp', 'ep'), may hold values from -0.125 to 0.125
- w_up: bfloat16 [2048, 16384], P('fsdp', 'ep'), may hold values from -0.125 to 0.125
- w_down: bfloat16 [16384, 2048], P('ep', 'fsdp'), may hold values from -0.0625 to 0.0625
Outputs:
- grad_tokens: bfloat16 [8192, 2048], P(('fsdp', 'ep'))
- route_dot: float32 [8192, 2], P(('fsdp', 'ep'))
- aux_grad: float32 [8192, 8], P(('fsdp', 'ep'))
- grad_gate: bfloat16 [2048, 16384], P('fsdp', 'ep')
- grad_up: bfloat16 [2048, 16384], P('fsdp', 'ep')
- grad_down: bfloat16 [16384, 2048], P('ep', 'fsdp')
The draws below stay inside these ranges and needn't reach their ends.
Inputs may be any that keep to these rules, and one draw needn't show every extreme that they name: `routes`: each token names two different experts; on every device at most 3 tokens name one expert, and some expert is named by exactly 3 of them.
All inputs are finite; a program needn't handle non-finite values.
Results may differ from the reference program's by a relative error of at most 0.04.
Values may be sent and summed in bfloat16 or wider, within the bound.
No kernel may reach another device: no remote copies, remote signals or barrier semaphores. Data moves between devices by JAX's collectives and lax.ppermute only.
A program may use at most 32 MiB of HBM per device.

```python
import jax
import jax.numpy as jnp
from jax import lax

D = 2048
FF = 8192
EXPERTS = 8
EXP_WIN = 2
TOK_DEV = 8
CAP = 3
TOKENS = 8192
N_FSDP = 16
N_EP = 64


def draw_routes(key, part):
    nblocks = TOKENS // TOK_DEV
    rank = jnp.arange(nblocks, dtype=jnp.int32)
    jitter = jax.random.randint(jax.random.fold_in(key, 11), (nblocks,), 0, 3, dtype=jnp.int32)
    offset = rank * 6 // nblocks + jitter
    places = jnp.arange(TOK_DEV, dtype=jnp.int32)
    first = offset[:, None] + places[None, :] // CAP
    second = offset[:, None] + (places[None, :] + TOK_DEV) // CAP
    paired = jnp.stack([first, second], axis=2) % EXPERTS
    scores = jax.random.randint(jax.random.fold_in(key, 12), (nblocks, TOK_DEV), 0, 1 << 20, dtype=jnp.int32) * TOK_DEV + places[None, :]
    order = jnp.argsort(scores, axis=1, stable=True).astype(jnp.int32)
    paired = jnp.take_along_axis(paired, order[:, :, None], axis=1)
    flipped = jax.random.randint(jax.random.fold_in(key, 13), (nblocks, TOK_DEV, 1), 0, 2, dtype=jnp.int32)
    paired = jnp.where(flipped == 1, paired[:, :, ::-1], paired)
    return paired.reshape(TOKENS, 2).astype(jnp.int32)


def shard_levels(key, shape, pieces, least, high):
    def one(axis_at, parts):
        draws = jax.random.uniform(jax.random.fold_in(jax.random.fold_in(key, 6), axis_at), (parts,), jnp.float32, least / len(pieces), high / len(pieces))
        return jnp.repeat(jnp.exp(draws), shape[axis_at] // parts).reshape((-1,) + (1,) * (len(shape) - axis_at - 1))

    level = one(*pieces[0])
    for cut in pieces[1:]:
        level = level * one(*cut)
    return level


def bell_draw(key, dims, scale, bound, pieces=(), held_as=jnp.bfloat16):
    result = scale * jax.random.normal(key, dims, jnp.float32)
    if pieces:
        result = result * shard_levels(key, dims, pieces, -0.22, 0.18)
    return jnp.clip(result, -bound, bound).astype(held_as)


def setup_inputs(seed: int = 0) -> dict:
    splits = jax.random.split(jax.random.key(seed), 8)
    tokens = bell_draw(splits[0], (TOKENS, D), 1.0, 6.0, ((0, 1024),))
    cotangent = bell_draw(splits[1], (TOKENS, D), 0.5, 4.0, ((0, 1024),))
    routes = draw_routes(jax.random.fold_in(splits[7], 71), 0)
    logits = bell_draw(splits[3], (TOKENS, EXPERTS), 2.0, 8.0, ((0, 1024),), jnp.float32)
    w_gate = bell_draw(splits[4], (D, EXP_WIN * FF), D ** -0.5, 0.125, ((0, 16), (1, 64)))
    w_up = bell_draw(splits[5], (D, EXP_WIN * FF), D ** -0.5, 0.125, ((0, 16), (1, 64)))
    w_down = bell_draw(splits[6], (EXP_WIN * FF, D), FF ** -0.5, 0.0625, ((0, 64), (1, 16)))
    return dict(tokens=tokens, cotangent=cotangent, routes=routes, logits=logits, w_gate=w_gate, w_up=w_up, w_down=w_down)


def routing(routes, logits):
    experts_all = logits.shape[-1]
    picked = (routes[:, :, None] == jnp.arange(experts_all, dtype=jnp.int32)[None, None, :]).astype(jnp.float32)
    chosen = jnp.sum(picked * logits[:, None, :], axis=2)
    combine = jax.nn.softmax(chosen, axis=1)
    window = picked[:, :, :EXP_WIN]
    member = jnp.sum(window, axis=1)
    scaled = jnp.sum(window * combine[:, :, None], axis=1)
    member_int = member.astype(jnp.int32)
    slot_ids = jnp.cumsum(member_int, axis=0) - member_int
    places = jnp.arange(CAP, dtype=jnp.int32)
    select = member[:, :, None] * (slot_ids[:, :, None] == places[None, None, :]).astype(jnp.float32)
    select = jnp.transpose(select, (1, 2, 0))
    slot_weight = jnp.einsum('xct,tx->xc', select, scaled)
    return select, slot_weight


def dispatch(select, slot_weight, tokens, cotangent):
    sent_tokens = jnp.einsum('xct,td->xcd', select, tokens.astype(jnp.float32)).astype(jnp.bfloat16)
    moved = jnp.einsum('xct,td->xcd', select, cotangent.astype(jnp.float32))
    sent_grads = (moved * slot_weight[:, :, None]).astype(jnp.bfloat16)
    return sent_tokens, sent_grads


def aux_gradient(routes, logits, total_counts):
    frac = total_counts.astype(jnp.float32) / jnp.sum(total_counts.astype(jnp.float32))
    probs = jax.nn.softmax(logits, axis=1)
    target = logits.shape[1] * frac
    return probs * (target[None, :] - jnp.sum(probs * target[None, :], axis=1, keepdims=True))


def expert_pass(rows_x, rows_dy, gate_w, up_w, down_w, blocks):
    gate_pre = jnp.dot(rows_x, gate_w, preferred_element_type=jnp.float32)
    up_pre = jnp.dot(rows_x, up_w, preferred_element_type=jnp.float32)
    sigma = jax.nn.sigmoid(gate_pre)
    active = gate_pre * sigma
    hidden = (active * up_pre).astype(jnp.bfloat16)
    hidden_grad = jnp.dot(rows_dy, down_w.T, preferred_element_type=jnp.float32)
    nrows = rows_x.shape[0]
    block_width = gate_w.shape[1] // blocks
    dots = jnp.sum((hidden.astype(jnp.float32) * hidden_grad).reshape(nrows, blocks, block_width), axis=2).astype(jnp.bfloat16)
    dots = jnp.sum(lax.optimization_barrier(dots).astype(jnp.float32), axis=1)
    up_grad = (hidden_grad * active).astype(jnp.bfloat16)
    gate_grad = (hidden_grad * up_pre * sigma * (1.0 + gate_pre * (1.0 - sigma))).astype(jnp.bfloat16)
    width_model = gate_w.shape[0]
    partial_value = jnp.einsum('rsf,dsf->srd', gate_grad.astype(jnp.float32).reshape(nrows, blocks, block_width),
                         gate_w.astype(jnp.float32).reshape(width_model, blocks, block_width))
    partial_value = partial_value + jnp.einsum('rsf,dsf->srd', up_grad.astype(jnp.float32).reshape(nrows, blocks, block_width),
                                   up_w.astype(jnp.float32).reshape(width_model, blocks, block_width))
    partial_value = lax.optimization_barrier(partial_value.astype(jnp.bfloat16))
    slot_grad = jnp.sum(partial_value.astype(jnp.float32), axis=0)
    grad_g = jnp.dot(rows_x.T, gate_grad, preferred_element_type=jnp.float32).astype(jnp.bfloat16)
    grad_u = jnp.dot(rows_x.T, up_grad, preferred_element_type=jnp.float32).astype(jnp.bfloat16)
    grad_d = jnp.dot(hidden.T, rows_dy, preferred_element_type=jnp.float32).astype(jnp.bfloat16)
    return slot_grad, dots, grad_g, grad_u, grad_d


def reference(tokens, cotangent, routes, logits, w_gate, w_up, w_down):
    blocks = N_EP // EXP_WIN
    tok = tokens.reshape(N_FSDP * N_EP, TOK_DEV, D)
    cot = cotangent.reshape(N_FSDP * N_EP, TOK_DEV, D)
    rts = routes.reshape(N_FSDP * N_EP, TOK_DEV, 2)
    lgt = logits.reshape(N_FSDP * N_EP, TOK_DEV, EXPERTS)
    select, slot_weight = jax.vmap(routing)(rts, lgt)
    sent_tokens, sent_grads = jax.vmap(dispatch)(select, slot_weight, tok, cot)
    sent_tokens = sent_tokens.reshape(N_FSDP, N_EP, EXP_WIN, CAP, D)
    sent_grads = sent_grads.reshape(N_FSDP, N_EP, EXP_WIN, CAP, D)

    def group_step(carry, blocks_in):
        acc_gate, acc_up, acc_down = carry
        group_x, group_dy = blocks_in
        grads_out = []
        dots_out = []
        for expert in range(EXP_WIN):
            low = expert * FF
            rows_x = group_x[:, expert].reshape(N_EP * CAP, D)
            rows_dy = group_dy[:, expert].reshape(N_EP * CAP, D)
            slot_grad, dots, grad_g, grad_u, grad_d = expert_pass(
                rows_x, rows_dy, w_gate[:, low:low + FF], w_up[:, low:low + FF], w_down[low:low + FF, :], blocks)
            acc_gate = acc_gate.at[:, low:low + FF].add(grad_g.astype(jnp.float32))
            acc_up = acc_up.at[:, low:low + FF].add(grad_u.astype(jnp.float32))
            acc_down = acc_down.at[low:low + FF, :].add(grad_d.astype(jnp.float32))
            grads_out.append(slot_grad.reshape(N_EP, CAP, D))
            dots_out.append(dots.reshape(N_EP, CAP))
        return (acc_gate, acc_up, acc_down), (jnp.stack(grads_out, axis=1), jnp.stack(dots_out, axis=1))

    start = (jnp.zeros((D, EXP_WIN * FF), jnp.float32), jnp.zeros((D, EXP_WIN * FF), jnp.float32),
             jnp.zeros((EXP_WIN * FF, D), jnp.float32))
    (acc_gate, acc_up, acc_down), (slot_grads, slot_dots) = lax.scan(group_step, start, (sent_tokens, sent_grads))
    slot_grads = slot_grads.reshape(N_FSDP * N_EP, EXP_WIN, CAP, D)
    slot_dots = slot_dots.reshape(N_FSDP * N_EP, EXP_WIN, CAP)
    grad_tokens = jnp.einsum('nxct,nxcd->ntd', select, slot_grads).reshape(TOKENS, D).astype(jnp.bfloat16)
    route_dot = jnp.einsum('nxct,nxc->ntx', select, slot_dots).reshape(TOKENS, EXP_WIN)
    total_counts = jnp.sum((routes[:, :, None] == jnp.arange(EXPERTS, dtype=jnp.int32)[None, None, :]).astype(jnp.int32), axis=(0, 1))
    aux_grad = aux_gradient(routes, logits, total_counts)
    return (grad_tokens, route_dot, aux_grad, acc_gate.astype(jnp.bfloat16), acc_up.astype(jnp.bfloat16),
            acc_down.astype(jnp.bfloat16))
```

```python
import jax
import jax.numpy as jnp
from jax import lax
from jax.experimental import pallas as pl
from jax.experimental.pallas import tpu as pltpu
from jax.sharding import Mesh
from jax.sharding import PartitionSpec as P

NX, NC, NZ, NY = 8, 2, 8, 8
ALL = ("x", "c", "z", "y")
SWAP = ((0, 1), (1, 0))
CAP = 3
DM = 2048
HID = 256
BLK = 128
NSRC = NZ * NY
WIRE = 1536
BACK = 896
SHARD = 3 * BLK + 8
ROWS = NSRC * CAP
VM = pl.BlockSpec(memory_space=pltpu.VMEM)
SM = pl.BlockSpec(memory_space=pltpu.SMEM)
bf16, f32, i32 = jnp.bfloat16, jnp.float32, jnp.int32
FIRST = (((0,), (0,)), ((), ()))
LAST = (((1,), (1,)), ((), ()))


def dot(a, b, dims=(((1,), (0,)), ((), ()))):
    return lax.dot_general(a, b, dims, preferred_element_type=f32)


def call(kernel, outs, n_in, name, scalars=True):
    specs = [VM] * n_in
    if scalars:
        specs = [SM] + specs
    return pl.pallas_call(
        kernel,
        out_shape=outs,
        in_specs=specs,
        out_specs=jax.tree.map(lambda _: VM, outs),
        name=name,
    )


def shape(*dims, dtype=bf16):
    return jax.ShapeDtypeStruct(dims, dtype)


def iota(dims, axis):
    return lax.broadcasted_iota(i32, dims, axis)


def slots(routes):
    lane = iota((8, 8), 1)
    pick0 = (routes[:, 0:1] == lane).astype(f32)
    pick1 = (routes[:, 1:2] == lane).astype(f32)
    member = pick0 + pick1
    below = (iota((8, 8), 1) < iota((8, 8), 0)).astype(f32)
    slot = dot(below, member)
    return pick0, pick1, member, slot


def own_first(v, core):
    even = [v[:, 256 * k : 256 * k + 128] for k in range(8)]
    odd = [v[:, 256 * k + 128 : 256 * k + 256] for k in range(8)]
    mine = [jnp.where(core == 0, a, b) for a, b in zip(even, odd)]
    rest = [jnp.where(core == 0, b, a) for a, b in zip(even, odd)]
    return jnp.concatenate(mine + rest, axis=1)


def in_order(v, core):
    mine = [v[:, 128 * k : 128 * k + 128] for k in range(8)]
    rest = [v[:, 1024 + 128 * k : 1152 + 128 * k] for k in range(8)]
    both = []
    for a, b in zip(mine, rest):
        both += [jnp.where(core == 0, a, b), jnp.where(core == 0, b, a)]
    return jnp.concatenate(both, axis=1)


def pack_weights(routes, w_gate, w_up, w_down, out):
    out[0:BLK] = w_gate[...]
    out[BLK : 2 * BLK] = w_up[...]
    out[2 * BLK : 3 * BLK] = jnp.transpose(w_down[...].astype(f32)).astype(bf16)
    lane = iota((8, HID), 1)
    hits = (routes[:, 0:1] == lane).astype(f32) + (routes[:, 1:2] == lane).astype(f32)
    total = jnp.sum(hits, axis=0, keepdims=True)
    row = iota((8, HID), 0)
    out[3 * BLK : SHARD] = jnp.where(row == 0, total, 0.0).astype(bf16)


def send_rows(idx, tokens, cotangent, routes, logits, out):
    core = idx[1]
    pick0, pick1, member, slot = slots(routes[...])
    lg = logits[...]
    l0 = jnp.sum(pick0 * lg, axis=1, keepdims=True)
    l1 = jnp.sum(pick1 * lg, axis=1, keepdims=True)
    top = jnp.maximum(l0, l1)
    e0, e1 = jnp.exp(l0 - top), jnp.exp(l1 - top)
    both = e0 + e1
    scaled = pick0 * (e0 / both) + pick1 * (e1 / both)
    tok = own_first(tokens[...].astype(f32), core)
    cot = own_first(cotangent[...].astype(f32), core)
    lane = iota((8, 8), 1)
    tok_b = tok.astype(bf16)
    for x in range(2):
        mem, at = member[:, x : x + 1], slot[:, x : x + 1].astype(i32)
        sel_x = jnp.where((at == lane) & (lane < CAP), mem, 0.0).astype(bf16)
        sel_g = jnp.where((at + CAP == lane) & (lane < 2 * CAP), mem, 0.0).astype(bf16)
        grads = (cot * scaled[:, x : x + 1]).astype(bf16)
        rows = dot(sel_x, tok_b, FIRST) + dot(sel_g, grads, FIRST)
        tail = rows[:, WIRE:].astype(bf16)
        pieces = []
        for r in range(CAP):
            to, fr = iota((8, 8), 0), iota((8, 8), 1)
            move = ((to == 6) & (fr == r)) | ((to == 7) & (fr == CAP + r))
            moved = dot(move.astype(f32).astype(bf16), tail)
            pieces.append((rows[:, 512 * r : 512 * r + 512] + moved).astype(bf16))
        block = jnp.concatenate(pieces, axis=1)
        out[32 * x : 32 * x + 32] = jnp.broadcast_to(block[None], (32, 8, WIRE))


def stack_shards(idx, *refs):
    out = refs[8]
    for k in range(8):
        out[lax.rem(idx[0] + 8 - k, 8)] = refs[k][...]


def one_hot(cond):
    return cond.astype(f32).astype(bf16)


def forward(wire, own, oth, x_out, g_out, grads_out, back):
    to, fr = iota((192, 256), 0), iota((192, 256), 1)
    main = one_hot(fr == 8 * (to & 31) + (to >> 5))
    to, fr = iota((64, 256), 0), iota((64, 256), 1)
    ends = one_hot(fr == 8 * (to & 31) + 6 + (to >> 5))
    for j in range(2):
        part = dot(main, wire[256 * j : 256 * j + 256, :]).astype(bf16)
        x_out[96 * j : 96 * j + 96, 0:WIRE] = part[0:96]
        g_out[96 * j : 96 * j + 96, 0:WIRE] = part[96:192]
        for r in range(CAP):
            at = 96 * j + 32 * r
            tail = dot(ends, wire[256 * j : 256 * j + 256, 512 * r : 512 * r + 512]).astype(bf16)
            x_out[at : at + 32, WIRE:DM] = tail[0:32]
            g_out[at : at + 32, WIRE:DM] = tail[32:64]
    half = DM // 2

    def weight(ref, k):
        return ref[:, k * BLK : (k + 1) * BLK, :].reshape(half, HID)

    def full(rows, k):
        return dot(rows[:, 0:half], weight(own, k)) + dot(rows[:, half:DM], weight(oth, k))

    gate_pre = full(x_out, 0)
    up_pre = full(x_out, 1)
    hidden_grad = full(g_out, 2)
    sigma = 1.0 / (1.0 + jnp.exp(-gate_pre))
    active = gate_pre * sigma
    hidden = (active * up_pre).astype(bf16)
    part_dot = jnp.sum(hidden.astype(f32) * hidden_grad, axis=1, keepdims=True)
    up_grad = (hidden_grad * active).astype(bf16)
    gate_grad = (hidden_grad * up_pre * sigma * (1.0 + gate_pre * (1.0 - sigma))).astype(bf16)
    grads_out[:, 0:HID] = gate_grad
    grads_out[:, HID : 2 * HID] = up_grad
    grads_out[:, 2 * HID : 3 * HID] = hidden
    counts = jnp.zeros((8, HID), f32)
    for k in range(8):
        counts = counts + own[k, 3 * BLK : SHARD, :].astype(f32)
        counts = counts + oth[k, 3 * BLK : SHARD, :].astype(f32)
    tally = jnp.sum(counts, axis=0, keepdims=True)[:, 0:BLK]
    px = []
    for ref in (own, oth):
        v = dot(gate_grad, weight(ref, 0), LAST) + dot(up_grad, weight(ref, 1), LAST)
        px.append(v.astype(bf16))
    to, fr = iota((256, 96), 0), iota((256, 96), 1)
    row, src, slot_of, src_of = to & 7, to >> 3, fr >> 5, fr & 31
    same = src == src_of
    first = one_hot(same & (row == 2 * slot_of))
    second = one_hot(same & (row == 2 * slot_of + 1))
    c60 = one_hot(same & (row == 6) & (slot_of == 0))
    c61 = one_hot(same & (row == 6) & (slot_of == 1))
    c71 = one_hot(same & (row == 7) & (slot_of == 1))
    c72 = one_hot(same & (row == 7) & (slot_of == 2))
    for_dot = one_hot(same & (row == slot_of))
    lane = iota((96, BLK), 1)
    count_at = (iota((256, BLK), 0) & 7) == CAP
    for j in range(2):

        def piece(k):
            v = px[k // 4]
            k = k % 4
            return v[96 * j : 96 * j + 96, 256 * k : 256 * k + 256]

        lo, hi = piece(6), piece(7)
        ends = ((c60, lo, c71, hi), (c60, hi, c72, lo), (c61, lo, c72, hi))
        for n in range(3):
            a, va, b, vb = ends[n]
            v = dot(first, piece(n)) + dot(second, piece(n + 3)) + dot(a, va) + dot(b, vb)
            back[256 * j : 256 * j + 256, 256 * n : 256 * n + 256] = v.astype(bf16)
        dots = jnp.where(lane == 0, part_dot[96 * j : 96 * j + 96], 0.0).astype(bf16)
        last = dot(for_dot, dots) + jnp.where(count_at, tally, 0.0)
        back[256 * j : 256 * j + 256, 768:BACK] = last.astype(bf16)


def weight_grads(x_rows, g_rows, grads, keep, send):
    half = DM // 2
    for ref, at in ((send, half), (keep, 0)):
        for k, rows in ((0, x_rows), (1, x_rows), (2, g_rows)):
            v = dot(rows[:, at : at + half], grads[:, k * HID : (k + 1) * HID], FIRST)
            ref[:, k * BLK : (k + 1) * BLK, :] = v.astype(bf16).reshape(8, BLK, HID)


def add_cores(idx, keep, came, *outs):
    for k in range(8):
        at = lax.rem(idx[0] + k, 8)
        outs[k][...] = (keep[at].astype(f32) + came[at].astype(f32)).astype(bf16)


def sum_chips(*refs):
    ins, (gate, up, down) = refs[:8], refs[8:]
    for k, ref in ((0, gate), (1, up), (2, down)):
        total = ins[0][k * BLK : (k + 1) * BLK].astype(f32)
        for i in range(1, 8):
            total = total + ins[i][k * BLK : (k + 1) * BLK].astype(f32)
        ref[...] = (jnp.transpose(total) if k == 2 else total).astype(bf16)


def finish(idx, back, routes, logits, grad_tokens, route_dot, aux_grad):
    core = idx[1]
    _, _, member, slot = slots(routes[...])
    total = jnp.zeros((8, DM), f32)
    counts = jnp.zeros((1, BLK), f32)
    dots = []
    for x in range(2):
        s = jnp.zeros((8, BACK), f32)
        for n in range(32):
            at = 8 * (32 * x + n)
            s = s + back[at : at + 8, :].astype(f32)
        counts = counts + s[CAP : CAP + 1, 768:BACK]
        at = slot[:, x : x + 1].astype(i32)
        ends = (
            s[6:7, 0:512],
            jnp.concatenate([s[6:7, 512:768], s[7:8, 0:256]], axis=1),
            s[7:8, 256:768],
        )
        dot_x = jnp.zeros((8, 1), f32)
        for r in range(CAP):
            sel = jnp.where(at == r, member[:, x : x + 1], 0.0)
            row = jnp.concatenate(
                [s[2 * r : 2 * r + 1, 0:768], s[2 * r + 1 : 2 * r + 2, 0:768], ends[r]], axis=1
            )
            total = total + sel * row
            dot_x = dot_x + sel * s[r : r + 1, 768:769]
        dots.append(dot_x)
    grad_tokens[...] = in_order(total, core).astype(bf16)
    lane2 = iota((8, 2), 1)
    route_dot[...] = jnp.where(lane2 == 0, dots[0], dots[1])
    lg = logits[...]
    e = jnp.exp(lg - jnp.max(lg, axis=1, keepdims=True))
    probs = e / jnp.sum(e, axis=1, keepdims=True)
    cnt = counts[:, 0:8]
    target = 8.0 * (cnt / jnp.sum(cnt, axis=1, keepdims=True))
    aux_grad[...] = probs * (target - jnp.sum(probs * target, axis=1, keepdims=True))


def shifted(value, by):
    return lax.ppermute(value, "x", [(i, (i + by) % NX) for i in range(NX)])


ORDER = (4, 3, 5, 2, 6, 1, 7)


def body(tokens, cotangent, routes, logits, w_gate, w_up, w_down):
    idx = jnp.stack([lax.axis_index("x"), lax.axis_index("c")]).astype(i32)
    wire = call(send_rows, shape(NSRC, 8, WIRE), 4, "send_rows")(
        idx, tokens, cotangent, routes, logits
    )
    shard = call(pack_weights, shape(SHARD, HID), 4, "pack_weights", False)(
        routes, w_gate, w_up, w_down
    )
    came = lax.all_to_all(wire, ("z", "y"), split_axis=0, concat_axis=0, tiled=True)
    parts = {0: shard}
    for k in ORDER:
        parts[k] = shifted(shard, k)
    own = call(stack_shards, shape(8, SHARD, HID), 8, "stack_shards")(
        idx, *[parts[k] for k in range(8)]
    )
    oth = lax.ppermute(own, "c", SWAP)
    x_rows, g_rows, grads, back = call(
        forward,
        (shape(ROWS, DM), shape(ROWS, DM), shape(ROWS, 3 * HID), shape(8 * NSRC, BACK)),
        3,
        "forward",
        False,
    )(came.reshape(8 * NSRC, WIRE), own, oth)
    keep, send = call(
        weight_grads, (shape(8, 3 * BLK, HID), shape(8, 3 * BLK, HID)), 3, "weight_grads", False
    )(x_rows, g_rows, grads)
    other = lax.ppermute(send, "c", SWAP)
    back = lax.all_to_all(
        back.reshape(NSRC, 8, BACK), ("z", "y"), split_axis=0, concat_axis=0, tiled=True
    )
    sums = call(add_cores, tuple(shape(3 * BLK, HID) for _ in range(8)), 2, "add_cores")(
        idx, keep, other
    )
    got = {0: sums[0]}
    for k in ORDER:
        got[k] = shifted(sums[k], k)
    grad_gate, grad_up, grad_down = call(
        sum_chips,
        (shape(BLK, HID), shape(BLK, HID), shape(HID, BLK)),
        8,
        "sum_chips",
        False,
    )(*[got[k] for k in range(8)])
    grad_tokens, route_dot, aux_grad = call(
        finish, (shape(8, DM), shape(8, 2, dtype=f32), shape(8, 8, dtype=f32)), 3, "finish"
    )(idx, back.reshape(8 * NSRC, BACK), routes, logits)
    return (grad_tokens, route_dot, aux_grad, grad_gate, grad_up, grad_down)


def solution(mesh):
    split = Mesh(mesh.devices.reshape(NX, NC, NZ, NY), ALL)
    rows, cols, down = P(ALL, None), P(("x", "c"), ("z", "y")), P(("z", "y"), ("x", "c"))
    return jax.shard_map(
        body,
        mesh=split,
        in_specs=(rows, rows, rows, rows, cols, cols, down),
        out_specs=(rows, rows, rows, cols, cols, down),
        check_vma=False,
    )
```

```python
import jax
import jax.numpy as jnp
from jax import lax
from jax.experimental import pallas as pl
from jax.experimental.pallas import tpu as pltpu
from jax.sharding import Mesh
from jax.sharding import PartitionSpec as P

NX, NC, NZ, NY = 8, 2, 8, 8
ALL = ("x", "c", "z", "y")
SWAP = ((0, 1), (1, 0))
CAP = 3
DM = 2048
HID = 256
BLK = 128
NSRC = NZ * NY
WIRE = 1536
BACK = 896
SHARD = 3 * BLK + 8
ROWS = NSRC * CAP
VM = pl.BlockSpec(memory_space=pltpu.VMEM)
bf16, f32, i32 = jnp.bfloat16, jnp.float32, jnp.int32
FIRST = (((0,), (0,)), ((), ()))
LAST = (((1,), (1,)), ((), ()))


def dot(a, b, dims=(((1,), (0,)), ((), ()))):
    return lax.dot_general(a, b, dims, preferred_element_type=f32)


def call(kernel, outs, n_in, name, limit=16):
    specs = [VM] * n_in
    return pl.pallas_call(
        kernel,
        out_shape=outs,
        in_specs=specs,
        out_specs=jax.tree.map(lambda _: VM, outs),
        name=name,
        compiler_params=pltpu.CompilerParams(vmem_limit_bytes=limit << 20),
    )


def shape(*dims, dtype=bf16):
    return jax.ShapeDtypeStruct(dims, dtype)


def iota(dims, axis):
    return lax.broadcasted_iota(i32, dims, axis)


def column(row):
    same = iota((8, 8), 0) == iota((8, 8), 1)
    return jnp.sum(jnp.where(same, row.astype(f32), 0.0), axis=1, keepdims=True)


def line(col):
    same = iota((8, 8), 0) == iota((8, 8), 1)
    return jnp.sum(jnp.where(same, col, 0.0), axis=0, keepdims=True)


def slots(routes_t):
    lane = iota((8, 8), 1).astype(f32)
    routes = (column(routes_t[0:1]), column(routes_t[1:2]))
    pick0 = (routes[0] == lane).astype(f32)
    pick1 = (routes[1] == lane).astype(f32)
    member = pick0 + pick1
    below = (iota((8, 8), 1) < iota((8, 8), 0)).astype(f32)
    slot = dot(below, member)
    return pick0, pick1, member, slot


def own_first(v, core):
    even = [v[:, 256 * k : 256 * k + 128] for k in range(8)]
    odd = [v[:, 256 * k + 128 : 256 * k + 256] for k in range(8)]
    mine = [jnp.where(core == 0, a, b) for a, b in zip(even, odd)]
    rest = [jnp.where(core == 0, b, a) for a, b in zip(even, odd)]
    return jnp.concatenate(mine + rest, axis=1)


def in_order(v, core):
    mine = [v[:, 128 * k : 128 * k + 128] for k in range(8)]
    rest = [v[:, 1024 + 128 * k : 1152 + 128 * k] for k in range(8)]
    both = []
    for a, b in zip(mine, rest):
        both += [jnp.where(core == 0, a, b), jnp.where(core == 0, b, a)]
    return jnp.concatenate(both, axis=1)


def pack_weights(routes, w_gate, w_up, w_down, out):
    out[0:BLK] = w_gate[...]
    out[BLK : 2 * BLK] = w_up[...]
    out[2 * BLK : 3 * BLK] = jnp.transpose(w_down[...].astype(f32)).astype(bf16)
    lane = iota((8, HID), 1).astype(f32)
    hits = (column(routes[0:1]) == lane).astype(f32) + (column(routes[1:2]) == lane).astype(f32)
    total = jnp.sum(hits, axis=0, keepdims=True)
    row = iota((8, HID), 0)
    out[3 * BLK : SHARD] = jnp.where(row == 0, total, 0.0).astype(bf16)


def send_rows(tokens, cotangent, routes, logits, out):
    core = lax.axis_index("c")
    pick0, pick1, member, slot = slots(routes[...])
    lg = logits[...]
    l0 = jnp.sum(pick0 * lg, axis=1, keepdims=True)
    l1 = jnp.sum(pick1 * lg, axis=1, keepdims=True)
    top = jnp.maximum(l0, l1)
    e0, e1 = jnp.exp(l0 - top), jnp.exp(l1 - top)
    both = e0 + e1
    scaled = pick0 * (e0 / both) + pick1 * (e1 / both)
    tok = own_first(tokens[...].astype(f32), core)
    cot = own_first(cotangent[...].astype(f32), core)
    lane = iota((8, 8), 1)
    tok_b = tok.astype(bf16)
    for x in range(2):
        mem, at = member[:, x : x + 1], slot[:, x : x + 1].astype(i32)
        sel_x = jnp.where((at == lane) & (lane < CAP), mem, 0.0).astype(bf16)
        sel_g = jnp.where((at + CAP == lane) & (lane < 2 * CAP), mem, 0.0).astype(bf16)
        grads = (cot * scaled[:, x : x + 1]).astype(bf16)
        rows = dot(sel_x, tok_b, FIRST) + dot(sel_g, grads, FIRST)
        tail = rows[:, WIRE:].astype(bf16)
        pieces = []
        for r in range(CAP):
            to, fr = iota((8, 8), 0), iota((8, 8), 1)
            move = ((to == 6) & (fr == r)) | ((to == 7) & (fr == CAP + r))
            moved = dot(move.astype(f32).astype(bf16), tail)
            pieces.append((rows[:, 512 * r : 512 * r + 512] + moved).astype(bf16))
        block = jnp.concatenate(pieces, axis=1)
        out[32 * x : 32 * x + 32] = jnp.broadcast_to(block[None], (32, 8, WIRE))


def stack_shards(*refs):
    out, chip = refs[8], lax.axis_index("x")
    for k in range(8):
        out[lax.rem(chip + 8 - k, 8)] = refs[k][...]


def one_hot(cond):
    return cond.astype(f32).astype(bf16)


def forward(wire, own, oth, x_out, g_out, grads_out, back):
    to, fr = iota((192, 256), 0), iota((192, 256), 1)
    main = one_hot(fr == 8 * (to & 31) + (to >> 5))
    to, fr = iota((64, 256), 0), iota((64, 256), 1)
    ends = one_hot(fr == 8 * (to & 31) + 6 + (to >> 5))
    for j in range(2):
        part = dot(main, wire[256 * j : 256 * j + 256, :]).astype(bf16)
        x_out[96 * j : 96 * j + 96, 0:WIRE] = part[0:96]
        g_out[96 * j : 96 * j + 96, 0:WIRE] = part[96:192]
        for r in range(CAP):
            at = 96 * j + 32 * r
            tail = dot(ends, wire[256 * j : 256 * j + 256, 512 * r : 512 * r + 512]).astype(bf16)
            x_out[at : at + 32, WIRE:DM] = tail[0:32]
            g_out[at : at + 32, WIRE:DM] = tail[32:64]
    half = DM // 2

    def weight(ref, k):
        return ref[:, k * BLK : (k + 1) * BLK, :].reshape(half, HID)

    def full(rows, k):
        return dot(rows[:, 0:half], weight(own, k)) + dot(rows[:, half:DM], weight(oth, k))

    gate_pre = full(x_out, 0)
    up_pre = full(x_out, 1)
    hidden_grad = full(g_out, 2)
    sigma = 1.0 / (1.0 + jnp.exp(-gate_pre))
    active = gate_pre * sigma
    hidden = (active * up_pre).astype(bf16)
    part_dot = jnp.sum(hidden.astype(f32) * hidden_grad, axis=1, keepdims=True)
    up_grad = (hidden_grad * active).astype(bf16)
    gate_grad = (hidden_grad * up_pre * sigma * (1.0 + gate_pre * (1.0 - sigma))).astype(bf16)
    grads_out[:, 0:HID] = gate_grad
    grads_out[:, HID : 2 * HID] = up_grad
    grads_out[:, 2 * HID : 3 * HID] = hidden
    counts = jnp.zeros((8, HID), f32)
    for k in range(8):
        counts = counts + own[k, 3 * BLK : SHARD, :].astype(f32)
        counts = counts + oth[k, 3 * BLK : SHARD, :].astype(f32)
    tally = jnp.sum(counts, axis=0, keepdims=True)[:, 0:BLK]
    px = []
    for ref in (own, oth):
        v = dot(gate_grad, weight(ref, 0), LAST) + dot(up_grad, weight(ref, 1), LAST)
        px.append(v.astype(bf16))
    to, fr = iota((256, 96), 0), iota((256, 96), 1)
    row, src, slot_of, src_of = to & 7, to >> 3, fr >> 5, fr & 31
    same = src == src_of
    first = one_hot(same & (row == 2 * slot_of))
    second = one_hot(same & (row == 2 * slot_of + 1))
    c60 = one_hot(same & (row == 6) & (slot_of == 0))
    c61 = one_hot(same & (row == 6) & (slot_of == 1))
    c71 = one_hot(same & (row == 7) & (slot_of == 1))
    c72 = one_hot(same & (row == 7) & (slot_of == 2))
    for_dot = one_hot(same & (row == slot_of))
    lane = iota((96, BLK), 1)
    count_at = (iota((256, BLK), 0) & 7) == CAP
    for j in range(2):

        def piece(k):
            v = px[k // 4]
            k = k % 4
            return v[96 * j : 96 * j + 96, 256 * k : 256 * k + 256]

        lo, hi = piece(6), piece(7)
        ends = ((c60, lo, c71, hi), (c60, hi, c72, lo), (c61, lo, c72, hi))
        for n in range(3):
            a, va, b, vb = ends[n]
            v = dot(first, piece(n)) + dot(second, piece(n + 3)) + dot(a, va) + dot(b, vb)
            back[256 * j : 256 * j + 256, 256 * n : 256 * n + 256] = v.astype(bf16)
        dots = jnp.where(lane == 0, part_dot[96 * j : 96 * j + 96], 0.0).astype(bf16)
        last = dot(for_dot, dots) + jnp.where(count_at, tally, 0.0)
        back[256 * j : 256 * j + 256, 768:BACK] = last.astype(bf16)


def weight_grads(x_rows, g_rows, grads, keep, send):
    half = DM // 2
    for ref, at in ((send, half), (keep, 0)):
        for k, rows in ((0, x_rows), (1, x_rows), (2, g_rows)):
            v = dot(rows[:, at : at + half], grads[:, k * HID : (k + 1) * HID], FIRST)
            ref[:, k * BLK : (k + 1) * BLK, :] = v.astype(bf16).reshape(8, BLK, HID)


def add_cores(keep, came, *outs):
    chip = lax.axis_index("x")
    for k in range(8):
        at = lax.rem(chip + k, 8)
        outs[k][...] = (keep[at].astype(f32) + came[at].astype(f32)).astype(bf16)


def join(*refs):
    s2, a, d, s6, b, t2, t6 = refs
    t2[...] = (s2[...].astype(f32) + a[...].astype(f32) + d[...].astype(f32)).astype(bf16)
    t6[...] = (s6[...].astype(f32) + b[...].astype(f32)).astype(bf16)


def sum_chips(*refs):
    ins, (gate, up, down) = refs[:5], refs[5:]
    for k, ref in ((0, gate), (1, up), (2, down)):
        total = ins[0][k * BLK : (k + 1) * BLK].astype(f32)
        for i in range(1, 5):
            total = total + ins[i][k * BLK : (k + 1) * BLK].astype(f32)
        ref[...] = (jnp.transpose(total) if k == 2 else total).astype(bf16)


def finish(back, routes, logits, grad_tokens, route_dot, aux_grad):
    core = lax.axis_index("c")
    _, _, member, slot = slots(routes[...])
    total = jnp.zeros((8, DM), f32)
    counts = jnp.zeros((1, BLK), f32)
    dots = []
    for x in range(2):
        s = jnp.zeros((8, BACK), f32)
        for n in range(32):
            at = 8 * (32 * x + n)
            s = s + back[at : at + 8, :].astype(f32)
        counts = counts + s[CAP : CAP + 1, 768:BACK]
        at = slot[:, x : x + 1].astype(i32)
        ends = (
            s[6:7, 0:512],
            jnp.concatenate([s[6:7, 512:768], s[7:8, 0:256]], axis=1),
            s[7:8, 256:768],
        )
        dot_x = jnp.zeros((8, 1), f32)
        for r in range(CAP):
            sel = jnp.where(at == r, member[:, x : x + 1], 0.0)
            row = jnp.concatenate(
                [s[2 * r : 2 * r + 1, 0:768], s[2 * r + 1 : 2 * r + 2, 0:768], ends[r]], axis=1
            )
            total = total + sel * row
            dot_x = dot_x + sel * s[r : r + 1, 768:769]
        dots.append(dot_x)
    grad_tokens[...] = in_order(total, core).astype(bf16)
    row2 = iota((2, 8), 0)
    route_dot[...] = jnp.where(row2 == 0, line(dots[0]), line(dots[1]))
    lg = logits[...]
    e = jnp.exp(lg - jnp.max(lg, axis=1, keepdims=True))
    probs = e / jnp.sum(e, axis=1, keepdims=True)
    cnt = counts[:, 0:8]
    target = 8.0 * (cnt / jnp.sum(cnt, axis=1, keepdims=True))
    aux_grad[...] = probs * (target - jnp.sum(probs * target, axis=1, keepdims=True))


def shifted(value, by):
    return lax.ppermute(value, "x", [(i, (i + by) % NX) for i in range(NX)])


def body(tokens, cotangent, routes, logits, w_gate, w_up, w_down):
    routes_t = routes.T
    wire = call(send_rows, shape(NSRC, 8, WIRE), 4, "send_rows")(
        tokens, cotangent, routes_t, logits
    )
    shard = call(pack_weights, shape(SHARD, HID), 4, "pack_weights")(routes_t, w_gate, w_up, w_down)
    came = lax.all_to_all(wire, ("z", "y"), split_axis=0, concat_axis=0, tiled=True)
    p2, m2 = shifted(shard, 2), shifted(shard, 6)
    p1, m1 = shifted(shard, 1), shifted(shard, 7)
    p4 = shifted(p2, 2)
    p3, m3 = shifted(p2, 1), shifted(m2, 7)
    own = call(stack_shards, shape(8, SHARD, HID), 8, "stack_shards")(
        shard, p1, p2, p3, p4, m3, m2, m1
    )
    oth = lax.ppermute(own, "c", SWAP)
    x_rows, g_rows, grads, back = call(
        forward,
        (shape(ROWS, DM), shape(ROWS, DM), shape(ROWS, 3 * HID), shape(8 * NSRC, BACK)),
        3,
        "forward",
    )(came.reshape(8 * NSRC, WIRE), own, oth)
    keep, send = call(
        weight_grads, (shape(8, 3 * BLK, HID), shape(8, 3 * BLK, HID)), 3, "weight_grads"
    )(x_rows, g_rows, grads)
    other = lax.ppermute(send, "c", SWAP)
    back = lax.all_to_all(
        back.reshape(NSRC, 8, BACK), ("z", "y"), split_axis=0, concat_axis=0, tiled=True
    )
    s = call(add_cores, tuple(shape(3 * BLK, HID) for _ in range(8)), 2, "add_cores")(keep, other)
    a, d, b = shifted(s[3], 1), shifted(s[4], 2), shifted(s[5], 7)
    e1, e7 = shifted(s[1], 1), shifted(s[7], 7)
    t2, t6 = call(join, (shape(3 * BLK, HID), shape(3 * BLK, HID)), 5, "join")(s[2], a, d, s[6], b)
    e2, e6 = shifted(t2, 2), shifted(t6, 6)
    grad_gate, grad_up, grad_down = call(
        sum_chips, (shape(BLK, HID), shape(BLK, HID), shape(HID, BLK)), 5, "sum_chips"
    )(s[0], e1, e7, e2, e6)
    grad_tokens, route_dot, aux_grad = call(
        finish, (shape(8, DM), shape(2, 8, dtype=f32), shape(8, 8, dtype=f32)), 3, "finish"
    )(back.reshape(8 * NSRC, BACK), routes_t, logits)
    return (grad_tokens, route_dot.T, aux_grad, grad_gate, grad_up, grad_down)


def solution(mesh):
    split = Mesh(mesh.devices.reshape(NX, NC, NZ, NY), ALL)
    rows, cols, down = P(ALL, None), P(("x", "c"), ("z", "y")), P(("z", "y"), ("x", "c"))
    return jax.shard_map(
        body,
        mesh=split,
        in_specs=(rows, rows, rows, rows, cols, cols, down),
        out_specs=(rows, rows, rows, cols, cols, down),
        check_vma=False,
    )
```

```python
import jax
import jax.numpy as jnp
from jax import lax
from jax.experimental import pallas as pl
from jax.experimental.pallas import tpu as pltpu
from jax.sharding import Mesh
from jax.sharding import PartitionSpec as P


NX, NC, NZ, NY = 8, 2, 8, 8
ALL = ("x", "c", "z", "y")
SWAP = ((0, 1), (1, 0))
CAP = 3
DM = 2048
HID = 256
BLK = 128
NSRC = NZ * NY
WIRE = 1536
BACK = 896
SHARD = 3 * BLK + 8
ROWS = NSRC * CAP
VM = pl.BlockSpec(memory_space=pltpu.VMEM)
FAR = pl.BlockSpec(memory_space=pltpu.HBM)
bf16, f32, i32 = jnp.bfloat16, jnp.float32, jnp.int32
FIRST = (((0,), (0,)), ((), ()))
LAST = (((1,), (1,)), ((), ()))


def dot(a, b, dims=(((1,), (0,)), ((), ()))):
    return lax.dot_general(a, b, dims, preferred_element_type=f32)


def call(kernel, outs, n_in, limit=16, far=(), scratch=()):
    specs = [FAR if k in far else VM for k in range(n_in)]
    return pl.pallas_call(
        kernel,
        out_shape=outs,
        in_specs=specs,
        out_specs=jax.tree.map(lambda _: VM, outs),
        scratch_shapes=scratch,
        compiler_params=pltpu.CompilerParams(vmem_limit_bytes=limit << 20),
    )


def shape(*dims, dtype=bf16):
    return jax.ShapeDtypeStruct(dims, dtype)


def iota(dims, axis):
    return lax.broadcasted_iota(i32, dims, axis)


def column(row):
    same = iota((8, 8), 0) == iota((8, 8), 1)
    return jnp.sum(jnp.where(same, row.astype(f32), 0.0), axis=1, keepdims=True)


def line(col):
    same = iota((8, 8), 0) == iota((8, 8), 1)
    return jnp.sum(jnp.where(same, col, 0.0), axis=0, keepdims=True)


def slots(routes_t):
    lane = iota((8, 8), 1).astype(f32)
    routes = (column(routes_t[0:1]), column(routes_t[1:2]))
    pick0 = (routes[0] == lane).astype(f32)
    pick1 = (routes[1] == lane).astype(f32)
    member = pick0 + pick1
    below = (iota((8, 8), 1) < iota((8, 8), 0)).astype(f32)
    slot = dot(below, member)
    return pick0, pick1, member, slot


def own_first(v, core):
    even = [v[:, 256 * k : 256 * k + 128] for k in range(8)]
    odd = [v[:, 256 * k + 128 : 256 * k + 256] for k in range(8)]
    mine = [jnp.where(core == 0, a, b) for a, b in zip(even, odd)]
    rest = [jnp.where(core == 0, b, a) for a, b in zip(even, odd)]
    return jnp.concatenate(mine + rest, axis=1)


def in_order(v, core):
    mine = [v[:, 128 * k : 128 * k + 128] for k in range(8)]
    rest = [v[:, 1024 + 128 * k : 1152 + 128 * k] for k in range(8)]
    both = []
    for a, b in zip(mine, rest):
        both += [jnp.where(core == 0, a, b), jnp.where(core == 0, b, a)]
    return jnp.concatenate(both, axis=1)


def pack_weights(routes, w_gate, w_up, w_down, out):
    out[0:BLK] = w_gate[...]
    out[BLK : 2 * BLK] = w_up[...]
    out[2 * BLK : 3 * BLK] = jnp.transpose(w_down[...].astype(f32)).astype(bf16)
    lane = iota((8, HID), 1)
    lane = jnp.where(lane < 16, lane & 7, 8).astype(f32)
    hits = (column(routes[0:1]) == lane).astype(f32) + (column(routes[1:2]) == lane).astype(f32)
    total = jnp.sum(hits, axis=0, keepdims=True)
    row = iota((8, HID), 0)
    out[3 * BLK : SHARD] = jnp.where(row == 0, total, 0.0).astype(bf16)


def send_rows(tokens, cotangent, routes, logits, out):
    core = lax.axis_index("c")
    pick0, pick1, member, slot = slots(routes[...])
    lg = logits[...]
    l0 = jnp.sum(pick0 * lg, axis=1, keepdims=True)
    l1 = jnp.sum(pick1 * lg, axis=1, keepdims=True)
    top = jnp.maximum(l0, l1)
    e0, e1 = jnp.exp(l0 - top), jnp.exp(l1 - top)
    both = e0 + e1
    scaled = pick0 * (e0 / both) + pick1 * (e1 / both)
    tok = own_first(tokens[...].astype(f32), core)
    cot = own_first(cotangent[...].astype(f32), core)
    lane = iota((8, 8), 1)
    tok_b = tok.astype(bf16)
    for x in range(2):
        mem, at = member[:, x : x + 1], slot[:, x : x + 1].astype(i32)
        sel_x = jnp.where((at == lane) & (lane < CAP), mem, 0.0).astype(bf16)
        sel_g = jnp.where((at + CAP == lane) & (lane < 2 * CAP), mem, 0.0).astype(bf16)
        grads = (cot * scaled[:, x : x + 1]).astype(bf16)
        rows = dot(sel_x, tok_b, FIRST) + dot(sel_g, grads, FIRST)
        tail = rows[:, WIRE:].astype(bf16)
        pieces = []
        for r in range(CAP):
            to, fr = iota((8, 8), 0), iota((8, 8), 1)
            move = ((to == 6) & (fr == r)) | ((to == 7) & (fr == CAP + r))
            moved = dot(move.astype(f32).astype(bf16), tail)
            pieces.append((rows[:, 512 * r : 512 * r + 512] + moved).astype(bf16))
        block = jnp.concatenate(pieces, axis=1)
        out[32 * x : 32 * x + 32] = jnp.broadcast_to(block[None], (32, 8, WIRE))


def stack_shards(*refs):
    out, chip = refs[8], lax.axis_index("x")
    for k in range(8):
        out[lax.rem(chip + 8 - k, 8)] = refs[k][...]


def one_hot(cond):
    return cond.astype(f32).astype(bf16)


def weight(ref, k):
    return ref[:, k * BLK : (k + 1) * BLK, :].reshape(DM // 2, HID)


def forward(wire, own, far, x_out, g_out, grads_out, dots_out, oth, sem):
    fetch = pltpu.make_async_copy(far, oth, sem)
    fetch.start()
    to, fr = iota((192, 256), 0), iota((192, 256), 1)
    main = one_hot(fr == 8 * (to & 31) + (to >> 5))
    to, fr = iota((64, 256), 0), iota((64, 256), 1)
    ends = one_hot(fr == 8 * (to & 31) + 6 + (to >> 5))
    for j in range(2):
        part = dot(main, wire[256 * j : 256 * j + 256, :]).astype(bf16)
        x_out[96 * j : 96 * j + 96, 0:WIRE] = part[0:96]
        g_out[96 * j : 96 * j + 96, 0:WIRE] = part[96:192]
        for r in range(CAP):
            at = 96 * j + 32 * r
            tail = dot(ends, wire[256 * j : 256 * j + 256, 512 * r : 512 * r + 512]).astype(bf16)
            x_out[at : at + 32, WIRE:DM] = tail[0:32]
            g_out[at : at + 32, WIRE:DM] = tail[32:64]
    half = DM // 2
    near = [dot(rows[:, 0:half], weight(own, k)) for k, rows in enumerate((x_out, x_out, g_out))]
    fetch.wait()
    gate_pre, up_pre, hidden_grad = [
        near[k] + dot(rows[:, half:DM], weight(oth, k))
        for k, rows in enumerate((x_out, x_out, g_out))
    ]
    sigma = 1.0 / (1.0 + jnp.exp(-gate_pre))
    active = gate_pre * sigma
    hidden = (active * up_pre).astype(bf16)
    part_dot = jnp.sum(hidden.astype(f32) * hidden_grad, axis=1, keepdims=True)
    up_grad = (hidden_grad * active).astype(bf16)
    gate_grad = (hidden_grad * up_pre * sigma * (1.0 + gate_pre * (1.0 - sigma))).astype(bf16)
    grads_out[:, 0:HID] = gate_grad
    grads_out[:, HID : 2 * HID] = up_grad
    grads_out[:, 2 * HID : 3 * HID] = hidden
    lane = iota((ROWS, BLK), 1)
    dots_out[...] = jnp.where(lane == 0, part_dot, 0.0).astype(bf16)


def row_grads(grads, dots, own, oth, back):
    gate_grad, up_grad = grads[:, 0:HID], grads[:, HID : 2 * HID]
    counts = jnp.zeros((8, HID), f32)
    for k in range(8):
        counts = counts + own[k, 3 * BLK : SHARD, :].astype(f32)
        counts = counts + oth[k, 3 * BLK : SHARD, :].astype(f32)
    tally = jnp.sum(counts, axis=0, keepdims=True)[:, 0:BLK]
    px = []
    for ref in (own, oth):
        v = dot(gate_grad, weight(ref, 0), LAST) + dot(up_grad, weight(ref, 1), LAST)
        px.append(v.astype(bf16))
    to, fr = iota((256, 96), 0), iota((256, 96), 1)
    row, slot_of = to & 7, fr >> 5
    same = 8 * ((to >> 3) & 3) + (to >> 5) == (fr & 31)
    first = one_hot(same & (row == 2 * slot_of))
    second = one_hot(same & (row == 2 * slot_of + 1))
    c60 = one_hot(same & (row == 6) & (slot_of == 0))
    c61 = one_hot(same & (row == 6) & (slot_of == 1))
    c71 = one_hot(same & (row == 7) & (slot_of == 1))
    c72 = one_hot(same & (row == 7) & (slot_of == 2))
    for_dot = one_hot(same & (row == slot_of))
    count_at = (iota((256, BLK), 0) & 7) == CAP
    for j in range(2):

        def piece(k):
            v = px[k // 4]
            k = k % 4
            return v[96 * j : 96 * j + 96, 256 * k : 256 * k + 256]

        def store(v, lo, hi):
            for y in range(8):
                at = 64 * y + 32 * j
                back[at : at + 32, lo:hi] = v[32 * y : 32 * y + 32]

        lo, hi = piece(6), piece(7)
        ends = ((c60, lo, c71, hi), (c60, hi, c72, lo), (c61, lo, c72, hi))
        for n in range(3):
            a, va, b, vb = ends[n]
            v = dot(first, piece(n)) + dot(second, piece(n + 3)) + dot(a, va) + dot(b, vb)
            store(v.astype(bf16), 256 * n, 256 * n + 256)
        last = dot(for_dot, dots[96 * j : 96 * j + 96, :]) + jnp.where(count_at, tally, 0.0)
        store(last.astype(bf16), 768, BACK)


def sum_y(came, out):
    s = came[0:64, :].astype(f32)
    for k in range(1, 8):
        s = s + came[64 * k : 64 * k + 64, :].astype(f32)
    out[:, 0:768] = s[:, 0:768].astype(bf16)
    last = s[:, 768:BACK]
    high = jnp.floor(last * 0.0625)
    digit = jnp.where(iota((64, BLK), 1) < 8, last - 16.0 * high, high)
    out[:, 768:BACK] = jnp.where((iota((64, BLK), 0) & 7) == CAP, digit, last).astype(bf16)


def weight_grads(x_rows, g_rows, grads, keep, send):
    half = DM // 2
    for ref, at in ((send, half), (keep, 0)):
        for k, rows in ((0, x_rows), (1, x_rows), (2, g_rows)):
            v = dot(rows[:, at : at + half], grads[:, k * HID : (k + 1) * HID], FIRST)
            ref[:, k * BLK : (k + 1) * BLK, :] = v.astype(bf16).reshape(8, BLK, HID)


def add_cores(keep, came, *outs):
    chip = lax.axis_index("x")
    for k in range(8):
        at = lax.rem(chip + k, 8)
        outs[k][...] = (keep[at].astype(f32) + came[at].astype(f32)).astype(bf16)


def join(*refs):
    s2, a, d, s6, b, t2, t6 = refs
    t2[...] = (s2[...].astype(f32) + a[...].astype(f32) + d[...].astype(f32)).astype(bf16)
    t6[...] = (s6[...].astype(f32) + b[...].astype(f32)).astype(bf16)


def sum_chips(*refs):
    ins, (gate, up, down) = refs[:5], refs[5:]
    for k, ref in ((0, gate), (1, up), (2, down)):
        total = ins[0][k * BLK : (k + 1) * BLK].astype(f32)
        for i in range(1, 5):
            total = total + ins[i][k * BLK : (k + 1) * BLK].astype(f32)
        ref[...] = (jnp.transpose(total) if k == 2 else total).astype(bf16)


def finish(back, routes, logits, grad_tokens, route_dot, aux_grad):
    core = lax.axis_index("c")
    _, _, member, slot = slots(routes[...])
    total = jnp.zeros((8, DM), f32)
    counts = jnp.zeros((1, BLK), f32)
    dots = []
    for x in range(2):
        s = jnp.zeros((8, BACK), f32)
        for n in range(4):
            at = 8 * (4 * x + n)
            s = s + back[at : at + 8, :].astype(f32)
        counts = counts + s[CAP : CAP + 1, 768:BACK]
        at = slot[:, x : x + 1].astype(i32)
        ends = (
            s[6:7, 0:512],
            jnp.concatenate([s[6:7, 512:768], s[7:8, 0:256]], axis=1),
            s[7:8, 256:768],
        )
        dot_x = jnp.zeros((8, 1), f32)
        for r in range(CAP):
            sel = jnp.where(at == r, member[:, x : x + 1], 0.0)
            row = jnp.concatenate(
                [s[2 * r : 2 * r + 1, 0:768], s[2 * r + 1 : 2 * r + 2, 0:768], ends[r]], axis=1
            )
            total = total + sel * row
            dot_x = dot_x + sel * s[r : r + 1, 768:769]
        dots.append(dot_x)
    grad_tokens[...] = in_order(total, core).astype(bf16)
    row2 = iota((2, 8), 0)
    route_dot[...] = jnp.where(row2 == 0, line(dots[0]), line(dots[1]))
    lg = logits[...]
    e = jnp.exp(lg - jnp.max(lg, axis=1, keepdims=True))
    probs = e / jnp.sum(e, axis=1, keepdims=True)
    cnt = counts[:, 0:8] + 16.0 * counts[:, 8:16]
    target = 8.0 * (cnt / jnp.sum(cnt, axis=1, keepdims=True))
    aux_grad[...] = probs * (target - jnp.sum(probs * target, axis=1, keepdims=True))


def shifted(value, by):
    return lax.ppermute(value, "x", [(i, (i + by) % NX) for i in range(NX)])


def exchange(value, axis):
    return lax.all_to_all(value, axis, split_axis=0, concat_axis=0, tiled=True)


def body(tokens, cotangent, routes, logits, w_gate, w_up, w_down):
    routes_t = routes.T
    shard = call(pack_weights, shape(SHARD, HID), 4, limit=60)(routes_t, w_gate, w_up, w_down)
    p2 = shifted(shard, 2)
    m2 = shifted(shard, 6)
    wire = call(send_rows, shape(NSRC, 8, WIRE), 4, limit=60)(tokens, cotangent, routes_t, logits)
    came = exchange(wire, ("z", "y"))
    p1 = shifted(shard, 1)
    m1 = shifted(shard, 7)
    p4 = shifted(p2, 2)
    p3 = shifted(p2, 1)
    m3 = shifted(m2, 7)
    own = call(stack_shards, shape(8, SHARD, HID), 8)(shard, p1, p2, p3, p4, m3, m2, m1)
    oth = lax.ppermute(own, "c", SWAP)
    x_rows, g_rows, grads, dots, oth = call(
        forward,
        (
            shape(ROWS, DM),
            shape(ROWS, DM),
            shape(ROWS, 3 * HID),
            shape(ROWS, BLK),
            shape(8, SHARD, HID),
        ),
        3,
        far=(2,),
        scratch=(pltpu.SemaphoreType.DMA,),
    )(came.reshape(8 * NSRC, WIRE), own, oth)
    keep, send = call(
        weight_grads, (shape(8, 3 * BLK, HID), shape(8, 3 * BLK, HID)), 3
    )(x_rows, g_rows, grads)
    other = lax.ppermute(send, "c", SWAP)
    back = call(row_grads, shape(8 * NSRC, BACK), 4)(grads, dots, own, oth)
    back = exchange(back.reshape(NY, 8 * NZ, BACK), "y")
    s = call(add_cores, tuple(shape(3 * BLK, HID) for _ in range(8)), 2)(keep, other)
    a, d, b = shifted(s[3], 1), shifted(s[4], 2), shifted(s[5], 7)
    e1 = shifted(s[1], 1)
    e7 = shifted(s[7], 7)
    t2, t6 = call(join, (shape(3 * BLK, HID), shape(3 * BLK, HID)), 5)(s[2], a, d, s[6], b)
    e2, e6 = shifted(t2, 2), shifted(t6, 6)
    back = call(sum_y, shape(8 * NZ, BACK), 1)(back.reshape(8 * NSRC, BACK))
    back = exchange(back.reshape(NZ, 8, BACK), "z")
    grad_gate, grad_up, grad_down = call(
        sum_chips, (shape(BLK, HID), shape(BLK, HID), shape(HID, BLK)), 5
    )(s[0], e1, e7, e2, e6)
    grad_tokens, route_dot, aux_grad = call(
        finish, (shape(8, DM), shape(2, 8, dtype=f32), shape(8, 8, dtype=f32)), 3
    )(back.reshape(8 * NZ, BACK), routes_t, logits)
    return (grad_tokens, route_dot.T, aux_grad, grad_gate, grad_up, grad_down)


def solution(mesh):
    split = Mesh(mesh.devices.reshape(NX, NC, NZ, NY), ALL)
    rows, cols, down = P(ALL, None), P(("x", "c"), ("z", "y")), P(("z", "y"), ("x", "c"))

    return jax.shard_map(
        body,
        mesh=split,
        in_specs=(rows, rows, rows, rows, cols, cols, down),
        out_specs=(rows, rows, rows, cols, cols, down),
        check_vma=False,
    )
```

```python
import jax
import jax.numpy as jnp
from jax import lax
from jax.experimental import pallas as pl
from jax.experimental.pallas import tpu as pltpu
from jax.sharding import Mesh
from jax.sharding import PartitionSpec as P


NX, NC, NZ, NY = 8, 2, 8, 8
ALL = ("x", "c", "z", "y")
SWAP = ((0, 1), (1, 0))
CAP = 3
DM = 2048
HID = 256
BLK = 128
NSRC = NZ * NY
WIRE = 1536
BACK = 896
SHARD = 3 * BLK + 8
ROWS = NSRC * CAP
VM = pl.BlockSpec(memory_space=pltpu.VMEM)
FAR = pl.BlockSpec(memory_space=pltpu.HBM)
bf16, f32, i32 = jnp.bfloat16, jnp.float32, jnp.int32
FIRST = (((0,), (0,)), ((), ()))
LAST = (((1,), (1,)), ((), ()))


def dot(a, b, dims=(((1,), (0,)), ((), ()))):
    return lax.dot_general(a, b, dims, preferred_element_type=f32)


def call(kernel, outs, n_in, limit=16, far=(), scratch=()):
    specs = [FAR if k in far else VM for k in range(n_in)]
    return pl.pallas_call(
        kernel,
        out_shape=outs,
        in_specs=specs,
        out_specs=jax.tree.map(lambda _: VM, outs),
        scratch_shapes=scratch,
        compiler_params=pltpu.CompilerParams(vmem_limit_bytes=limit << 20),
    )


def shape(*dims, dtype=bf16):
    return jax.ShapeDtypeStruct(dims, dtype)


def iota(dims, axis):
    return lax.broadcasted_iota(i32, dims, axis)


def column(row):
    same = iota((8, 8), 0) == iota((8, 8), 1)
    return jnp.sum(jnp.where(same, row.astype(f32), 0.0), axis=1, keepdims=True)


def line(col):
    same = iota((8, 8), 0) == iota((8, 8), 1)
    return jnp.sum(jnp.where(same, col, 0.0), axis=0, keepdims=True)


def slots(routes_t):
    lane = iota((8, 8), 1).astype(f32)
    routes = (column(routes_t[0:1]), column(routes_t[1:2]))
    pick0 = (routes[0] == lane).astype(f32)
    pick1 = (routes[1] == lane).astype(f32)
    member = pick0 + pick1
    below = (iota((8, 8), 1) < iota((8, 8), 0)).astype(f32)
    slot = dot(below, member)
    return pick0, pick1, member, slot


def own_first(v, core):
    even = [v[:, 256 * k : 256 * k + 128] for k in range(8)]
    odd = [v[:, 256 * k + 128 : 256 * k + 256] for k in range(8)]
    mine = [jnp.where(core == 0, a, b) for a, b in zip(even, odd)]
    rest = [jnp.where(core == 0, b, a) for a, b in zip(even, odd)]
    return jnp.concatenate(mine + rest, axis=1)


def in_order(v, core):
    mine = [v[:, 128 * k : 128 * k + 128] for k in range(8)]
    rest = [v[:, 1024 + 128 * k : 1152 + 128 * k] for k in range(8)]
    both = []
    for a, b in zip(mine, rest):
        both += [jnp.where(core == 0, a, b), jnp.where(core == 0, b, a)]
    return jnp.concatenate(both, axis=1)


def pack_weights(routes, w_gate, w_up, w_down, out):
    out[0:BLK] = w_gate[...]
    out[BLK : 2 * BLK] = w_up[...]
    out[2 * BLK : 3 * BLK] = jnp.transpose(w_down[...].astype(f32)).astype(bf16)
    lane = iota((8, HID), 1).astype(f32)
    hits = (column(routes[0:1]) == lane).astype(f32) + (column(routes[1:2]) == lane).astype(f32)
    total = jnp.sum(hits, axis=0, keepdims=True)
    row = iota((8, HID), 0)
    out[3 * BLK : SHARD] = jnp.where(row == 0, total, 0.0).astype(bf16)


def send_rows(tokens, cotangent, routes, logits, out):
    core = lax.axis_index("c")
    pick0, pick1, member, slot = slots(routes[...])
    lg = logits[...]
    l0 = jnp.sum(pick0 * lg, axis=1, keepdims=True)
    l1 = jnp.sum(pick1 * lg, axis=1, keepdims=True)
    top = jnp.maximum(l0, l1)
    e0, e1 = jnp.exp(l0 - top), jnp.exp(l1 - top)
    both = e0 + e1
    scaled = pick0 * (e0 / both) + pick1 * (e1 / both)
    tok = own_first(tokens[...].astype(f32), core)
    cot = own_first(cotangent[...].astype(f32), core)
    lane = iota((8, 8), 1)
    tok_b = tok.astype(bf16)
    for x in range(2):
        mem, at = member[:, x : x + 1], slot[:, x : x + 1].astype(i32)
        sel_x = jnp.where((at == lane) & (lane < CAP), mem, 0.0).astype(bf16)
        sel_g = jnp.where((at + CAP == lane) & (lane < 2 * CAP), mem, 0.0).astype(bf16)
        grads = (cot * scaled[:, x : x + 1]).astype(bf16)
        rows = dot(sel_x, tok_b, FIRST) + dot(sel_g, grads, FIRST)
        tail = rows[:, WIRE:].astype(bf16)
        pieces = []
        for r in range(CAP):
            to, fr = iota((8, 8), 0), iota((8, 8), 1)
            move = ((to == 6) & (fr == r)) | ((to == 7) & (fr == CAP + r))
            moved = dot(move.astype(f32).astype(bf16), tail)
            pieces.append((rows[:, 512 * r : 512 * r + 512] + moved).astype(bf16))
        block = jnp.concatenate(pieces, axis=1)
        out[32 * x : 32 * x + 32] = jnp.broadcast_to(block[None], (32, 8, WIRE))


def stack_shards(*refs):
    out, chip = refs[8], lax.axis_index("x")
    for k in range(8):
        out[lax.rem(chip + 8 - k, 8)] = refs[k][...]


def one_hot(cond):
    return cond.astype(f32).astype(bf16)


def weight(ref, k):
    return ref[:, k * BLK : (k + 1) * BLK, :].reshape(DM // 2, HID)


def forward(wire, own, far, x_out, g_out, grads_out, dots_out, oth, sem):
    fetch = pltpu.make_async_copy(far, oth, sem)
    fetch.start()
    to, fr = iota((192, 256), 0), iota((192, 256), 1)
    main = one_hot(fr == 8 * (to & 31) + (to >> 5))
    to, fr = iota((64, 256), 0), iota((64, 256), 1)
    ends = one_hot(fr == 8 * (to & 31) + 6 + (to >> 5))
    for j in range(2):
        part = dot(main, wire[256 * j : 256 * j + 256, :]).astype(bf16)
        x_out[96 * j : 96 * j + 96, 0:WIRE] = part[0:96]
        g_out[96 * j : 96 * j + 96, 0:WIRE] = part[96:192]
        for r in range(CAP):
            at = 96 * j + 32 * r
            tail = dot(ends, wire[256 * j : 256 * j + 256, 512 * r : 512 * r + 512]).astype(bf16)
            x_out[at : at + 32, WIRE:DM] = tail[0:32]
            g_out[at : at + 32, WIRE:DM] = tail[32:64]
    half = DM // 2
    near = [dot(rows[:, 0:half], weight(own, k)) for k, rows in enumerate((x_out, x_out, g_out))]
    fetch.wait()
    gate_pre, up_pre, hidden_grad = [
        near[k] + dot(rows[:, half:DM], weight(oth, k))
        for k, rows in enumerate((x_out, x_out, g_out))
    ]
    sigma = 1.0 / (1.0 + jnp.exp(-gate_pre))
    active = gate_pre * sigma
    hidden = (active * up_pre).astype(bf16)
    part_dot = jnp.sum(hidden.astype(f32) * hidden_grad, axis=1, keepdims=True)
    up_grad = (hidden_grad * active).astype(bf16)
    gate_grad = (hidden_grad * up_pre * sigma * (1.0 + gate_pre * (1.0 - sigma))).astype(bf16)
    grads_out[:, 0:HID] = gate_grad
    grads_out[:, HID : 2 * HID] = up_grad
    grads_out[:, 2 * HID : 3 * HID] = hidden
    lane = iota((ROWS, BLK), 1)
    dots_out[...] = jnp.where(lane == 0, part_dot, 0.0).astype(bf16)


def row_grads(grads, dots, own, oth, back):
    gate_grad, up_grad = grads[:, 0:HID], grads[:, HID : 2 * HID]
    counts = jnp.zeros((8, HID), f32)
    for k in range(8):
        counts = counts + own[k, 3 * BLK : SHARD, :].astype(f32)
        counts = counts + oth[k, 3 * BLK : SHARD, :].astype(f32)
    tally = jnp.sum(counts, axis=0, keepdims=True)[:, 0:BLK]
    px = []
    for ref in (own, oth):
        v = dot(gate_grad, weight(ref, 0), LAST) + dot(up_grad, weight(ref, 1), LAST)
        px.append(v.astype(bf16))
    to, fr = iota((256, 96), 0), iota((256, 96), 1)
    row, slot_of = to & 7, fr >> 5
    same = (to >> 3) == (fr & 31)
    first = one_hot(same & (row == 2 * slot_of))
    second = one_hot(same & (row == 2 * slot_of + 1))
    c60 = one_hot(same & (row == 6) & (slot_of == 0))
    c61 = one_hot(same & (row == 6) & (slot_of == 1))
    c71 = one_hot(same & (row == 7) & (slot_of == 1))
    c72 = one_hot(same & (row == 7) & (slot_of == 2))
    for_dot = one_hot(same & (row == slot_of))
    count_at = (iota((256, BLK), 0) & 7) == CAP
    for j in range(2):

        def piece(k):
            v = px[k // 4]
            k = k % 4
            return v[96 * j : 96 * j + 96, 256 * k : 256 * k + 256]

        lo, hi = piece(6), piece(7)
        ends = ((c60, lo, c71, hi), (c60, hi, c72, lo), (c61, lo, c72, hi))
        for n in range(3):
            a, va, b, vb = ends[n]
            v = dot(first, piece(n)) + dot(second, piece(n + 3)) + dot(a, va) + dot(b, vb)
            back[256 * j : 256 * j + 256, 256 * n : 256 * n + 256] = v.astype(bf16)
        last = dot(for_dot, dots[96 * j : 96 * j + 96, :]) + jnp.where(count_at, tally, 0.0)
        back[256 * j : 256 * j + 256, 768:BACK] = last.astype(bf16)


def weight_grads(x_rows, g_rows, grads, keep, send):
    half = DM // 2
    for ref, at in ((send, half), (keep, 0)):
        for k, rows in ((0, x_rows), (1, x_rows), (2, g_rows)):
            v = dot(rows[:, at : at + half], grads[:, k * HID : (k + 1) * HID], FIRST)
            ref[:, k * BLK : (k + 1) * BLK, :] = v.astype(bf16).reshape(8, BLK, HID)


def add_cores(keep, came, s0, s2, s4, s6, right, left):
    chip = lax.axis_index("x")

    def total(k):
        at = lax.rem(chip + k, 8)
        return (keep[at].astype(f32) + came[at].astype(f32)).astype(bf16)

    right[0 : 3 * BLK] = total(3)
    right[3 * BLK :] = total(1)
    s4[...] = total(4)
    left[0 : 3 * BLK] = total(5)
    left[3 * BLK :] = total(7)
    s2[...] = total(2)
    s6[...] = total(6)
    s0[...] = total(0)


def join(s2, right, s4, s6, left, t2, t6):
    far = slice(0, 3 * BLK)
    t2[...] = (s2[...].astype(f32) + right[far].astype(f32) + s4[...].astype(f32)).astype(bf16)
    t6[...] = (s6[...].astype(f32) + left[far].astype(f32)).astype(bf16)


def sum_chips(s0, right, left, t2, t6, gate, up, down):
    for k, ref in ((0, gate), (1, up), (2, down)):
        lo, hi = k * BLK, (k + 1) * BLK
        total = s0[lo:hi].astype(f32) + t2[lo:hi].astype(f32) + t6[lo:hi].astype(f32)
        lo, hi = lo + 3 * BLK, hi + 3 * BLK
        total = total + right[lo:hi].astype(f32) + left[lo:hi].astype(f32)
        ref[...] = (jnp.transpose(total) if k == 2 else total).astype(bf16)


def finish(back, routes, logits, grad_tokens, route_dot, aux_grad):
    core = lax.axis_index("c")
    _, _, member, slot = slots(routes[...])
    total = jnp.zeros((8, DM), f32)
    counts = jnp.zeros((1, BLK), f32)
    dots = []
    for x in range(2):
        s = jnp.zeros((8, BACK), f32)
        for n in range(32):
            at = 8 * (32 * x + n)
            s = s + back[at : at + 8, :].astype(f32)
        counts = counts + s[CAP : CAP + 1, 768:BACK]
        at = slot[:, x : x + 1].astype(i32)
        ends = (
            s[6:7, 0:512],
            jnp.concatenate([s[6:7, 512:768], s[7:8, 0:256]], axis=1),
            s[7:8, 256:768],
        )
        dot_x = jnp.zeros((8, 1), f32)
        for r in range(CAP):
            sel = jnp.where(at == r, member[:, x : x + 1], 0.0)
            row = jnp.concatenate(
                [s[2 * r : 2 * r + 1, 0:768], s[2 * r + 1 : 2 * r + 2, 0:768], ends[r]], axis=1
            )
            total = total + sel * row
            dot_x = dot_x + sel * s[r : r + 1, 768:769]
        dots.append(dot_x)
    grad_tokens[...] = in_order(total, core).astype(bf16)
    row2 = iota((2, 8), 0)
    route_dot[...] = jnp.where(row2 == 0, line(dots[0]), line(dots[1]))
    lg = logits[...]
    e = jnp.exp(lg - jnp.max(lg, axis=1, keepdims=True))
    probs = e / jnp.sum(e, axis=1, keepdims=True)
    cnt = counts[:, 0:8]
    target = 8.0 * (cnt / jnp.sum(cnt, axis=1, keepdims=True))
    aux_grad[...] = probs * (target - jnp.sum(probs * target, axis=1, keepdims=True))


def shifted(value, by):
    return lax.ppermute(value, "x", [(i, (i + by) % NX) for i in range(NX)])


def exchange(value, axis):
    return lax.all_to_all(value, axis, split_axis=0, concat_axis=0, tiled=True)


def body(tokens, cotangent, routes, logits, w_gate, w_up, w_down):
    routes_t = routes.T
    shard = call(pack_weights, shape(SHARD, HID), 4, limit=60)(routes_t, w_gate, w_up, w_down)
    p2 = shifted(shard, 2)
    m2 = shifted(shard, 6)
    wire = call(send_rows, shape(NSRC, 8, WIRE), 4, limit=60)(tokens, cotangent, routes_t, logits)
    came = exchange(wire, ("z", "y"))
    p1 = shifted(shard, 1)
    m1 = shifted(shard, 7)
    p4 = shifted(p2, 2)
    p3 = shifted(p2, 1)
    m3 = shifted(m2, 7)
    own = call(stack_shards, shape(8, SHARD, HID), 8)(shard, p1, p2, p3, p4, m3, m2, m1)
    oth = lax.ppermute(own, "c", SWAP)
    x_rows, g_rows, grads, dots, oth = call(
        forward,
        (
            shape(ROWS, DM),
            shape(ROWS, DM),
            shape(ROWS, 3 * HID),
            shape(ROWS, BLK),
            shape(8, SHARD, HID),
        ),
        3,
        far=(2,),
        scratch=(pltpu.SemaphoreType.DMA,),
    )(came.reshape(8 * NSRC, WIRE), own, oth)
    keep, send = call(
        weight_grads, (shape(8, 3 * BLK, HID), shape(8, 3 * BLK, HID)), 3
    )(x_rows, g_rows, grads)
    other = lax.ppermute(send, "c", SWAP)
    back = call(row_grads, shape(8 * NSRC, BACK), 4)(grads, dots, own, oth)
    one, two = shape(3 * BLK, HID), shape(6 * BLK, HID)
    s0, s2, s4, s6, right, left = call(add_cores, (one, one, one, one, two, two), 2)(keep, other)
    right = shifted(right, 1)
    s4 = shifted(s4, 2)
    left = shifted(left, 7)
    back = exchange(back.reshape(NSRC, 8, BACK), ("z", "y"))
    t2, t6 = call(join, (one, one), 5)(s2, right, s4, s6, left)
    t2, t6 = shifted(t2, 2), shifted(t6, 6)
    grad_gate, grad_up, grad_down = call(
        sum_chips, (shape(BLK, HID), shape(BLK, HID), shape(HID, BLK)), 5
    )(s0, right, left, t2, t6)
    grad_tokens, route_dot, aux_grad = call(
        finish, (shape(8, DM), shape(2, 8, dtype=f32), shape(8, 8, dtype=f32)), 3
    )(back.reshape(8 * NSRC, BACK), routes_t, logits)
    return (grad_tokens, route_dot.T, aux_grad, grad_gate, grad_up, grad_down)


def solution(mesh):
    split = Mesh(mesh.devices.reshape(NX, NC, NZ, NY), ALL)
    rows, cols, down = P(ALL, None), P(("x", "c"), ("z", "y")), P(("z", "y"), ("x", "c"))

    return jax.shard_map(
        body,
        mesh=split,
        in_specs=(rows, rows, rows, rows, cols, cols, down),
        out_specs=(rows, rows, rows, cols, cols, down),
        check_vma=False,
    )
```

```python
import jax
import jax.numpy as jnp
from jax import lax
from jax.experimental import pallas as pl
from jax.experimental.pallas import tpu as pltpu
from jax.sharding import Mesh
from jax.sharding import PartitionSpec as P


NX, NC, NZ, NY = 8, 2, 8, 8
ALL = ("x", "c", "z", "y")
SWAP = ((0, 1), (1, 0))
CAP = 3
DM = 2048
HID = 256
BLK = 128
NSRC = NZ * NY
BACK = 896
SHARD = 3 * BLK + 8
ROWS = NSRC * CAP
HELD = (2, 6)
VM = pl.BlockSpec(memory_space=pltpu.VMEM)
FAR = pl.BlockSpec(memory_space=pltpu.HBM)
bf16, f32, i32 = jnp.bfloat16, jnp.float32, jnp.int32
FIRST = (((0,), (0,)), ((), ()))
LAST = (((1,), (1,)), ((), ()))


def dot(a, b, dims=(((1,), (0,)), ((), ()))):
    return lax.dot_general(a, b, dims, preferred_element_type=f32)


def call(kernel, outs, n_in, limit=16, far=(), scratch=()):
    specs = [FAR if k in far else VM for k in range(n_in)]
    return pl.pallas_call(
        kernel,
        out_shape=outs,
        in_specs=specs,
        out_specs=jax.tree.map(lambda _: VM, outs),
        scratch_shapes=scratch,
        compiler_params=pltpu.CompilerParams(vmem_limit_bytes=limit << 20),
    )


def shape(*dims, dtype=bf16):
    return jax.ShapeDtypeStruct(dims, dtype)


def iota(dims, axis):
    return lax.broadcasted_iota(i32, dims, axis)


def column(row):
    same = iota((8, 8), 0) == iota((8, 8), 1)
    return jnp.sum(jnp.where(same, row.astype(f32), 0.0), axis=1, keepdims=True)


def line(col):
    same = iota((8, 8), 0) == iota((8, 8), 1)
    return jnp.sum(jnp.where(same, col, 0.0), axis=0, keepdims=True)


def slots(routes_t):
    lane = iota((8, 8), 1).astype(f32)
    routes = (column(routes_t[0:1]), column(routes_t[1:2]))
    pick0 = (routes[0] == lane).astype(f32)
    pick1 = (routes[1] == lane).astype(f32)
    member = pick0 + pick1
    below = (iota((8, 8), 1) < iota((8, 8), 0)).astype(f32)
    slot = dot(below, member)
    return pick0, pick1, member, slot


def own_first(v, core):
    even = [v[:, 256 * k : 256 * k + 128] for k in range(8)]
    odd = [v[:, 256 * k + 128 : 256 * k + 256] for k in range(8)]
    mine = [jnp.where(core == 0, a, b) for a, b in zip(even, odd)]
    rest = [jnp.where(core == 0, b, a) for a, b in zip(even, odd)]
    return jnp.concatenate(mine + rest, axis=1)


def in_order(v, core):
    mine = [v[:, 128 * k : 128 * k + 128] for k in range(8)]
    rest = [v[:, 1024 + 128 * k : 1152 + 128 * k] for k in range(8)]
    both = []
    for a, b in zip(mine, rest):
        both += [jnp.where(core == 0, a, b), jnp.where(core == 0, b, a)]
    return jnp.concatenate(both, axis=1)


def pack_weights(routes, w_gate, w_up, w_down, out):
    out[0:BLK] = w_gate[...]
    out[BLK : 2 * BLK] = w_up[...]
    out[2 * BLK : 3 * BLK] = jnp.transpose(w_down[...].astype(f32)).astype(bf16)
    lane = iota((8, HID), 1).astype(f32)
    hits = (column(routes[0:1]) == lane).astype(f32) + (column(routes[1:2]) == lane).astype(f32)
    total = jnp.sum(hits, axis=0, keepdims=True)
    row = iota((8, HID), 0)
    out[3 * BLK : SHARD] = jnp.where(row == 0, total, 0.0).astype(bf16)


def send_rows(tokens, cotangent, routes, logits, out):
    core = lax.axis_index("c")
    pick0, pick1, member, slot = slots(routes[...])
    lg = logits[...]
    l0 = jnp.sum(pick0 * lg, axis=1, keepdims=True)
    l1 = jnp.sum(pick1 * lg, axis=1, keepdims=True)
    top = jnp.maximum(l0, l1)
    e0, e1 = jnp.exp(l0 - top), jnp.exp(l1 - top)
    both = e0 + e1
    scaled = pick0 * (e0 / both) + pick1 * (e1 / both)
    tok = own_first(tokens[...].astype(f32), core)
    cot = own_first(cotangent[...].astype(f32), core)
    lane = iota((8, 8), 1)
    tok_b = tok.astype(bf16)
    for x in range(2):
        mem, at = member[:, x : x + 1], slot[:, x : x + 1].astype(i32)
        sel_x = jnp.where((at == lane) & (lane < CAP), mem, 0.0).astype(bf16)
        sel_g = jnp.where((at + CAP == lane) & (lane < 2 * CAP), mem, 0.0).astype(bf16)
        grads = (cot * scaled[:, x : x + 1]).astype(bf16)
        block = (dot(sel_x, tok_b, FIRST) + dot(sel_g, grads, FIRST)).astype(bf16)
        out[4 * x : 4 * x + 4] = jnp.broadcast_to(block[None], (4, 8, DM))


def repack(came, out):
    to, fr = iota((48, 64), 0), iota((48, 64), 1)
    block = dot(one_hot(fr == 8 * (to & 7) + (to >> 3)), came[...]).astype(bf16)
    out[...] = jnp.broadcast_to(block[None], (NY, 48, DM))


def stack_shards(*refs):
    out, sem, chip = refs[8], refs[9], lax.axis_index("x")
    fetches = []
    for n, k in enumerate(HELD):
        at = lax.rem(chip + 8 - k, 8)
        fetches.append(pltpu.make_async_copy(refs[k], out.at[at], sem.at[n]))
        fetches[-1].start()
    for k in range(8):
        if k not in HELD:
            out[lax.rem(chip + 8 - k, 8)] = refs[k][...]
    for fetch in fetches:
        fetch.wait()


def one_hot(cond):
    return cond.astype(f32).astype(bf16)


def weight(ref, k):
    return ref[:, k * BLK : (k + 1) * BLK, :].reshape(DM // 2, HID)


def unpack(came, x_out, g_out):
    for y in range(NY):
        x_out[24 * y : 24 * y + 24] = came[48 * y : 48 * y + 24]
        g_out[24 * y : 24 * y + 24] = came[48 * y + 24 : 48 * y + 48]


def forward(x_rows, g_rows, own, far, grads_out, dots_out, oth, sem):
    fetch = pltpu.make_async_copy(far, oth, sem)
    fetch.start()
    half = DM // 2
    near = [dot(rows[:, 0:half], weight(own, k)) for k, rows in enumerate((x_rows, x_rows, g_rows))]
    fetch.wait()
    gate_pre, up_pre, hidden_grad = [
        near[k] + dot(rows[:, half:DM], weight(oth, k))
        for k, rows in enumerate((x_rows, x_rows, g_rows))
    ]
    sigma = 1.0 / (1.0 + jnp.exp(-gate_pre))
    active = gate_pre * sigma
    hidden = (active * up_pre).astype(bf16)
    part_dot = jnp.sum(hidden.astype(f32) * hidden_grad, axis=1, keepdims=True)
    up_grad = (hidden_grad * active).astype(bf16)
    gate_grad = (hidden_grad * up_pre * sigma * (1.0 + gate_pre * (1.0 - sigma))).astype(bf16)
    grads_out[:, 0:HID] = gate_grad
    grads_out[:, HID : 2 * HID] = up_grad
    grads_out[:, 2 * HID : 3 * HID] = hidden
    lane = iota((ROWS, BLK), 1)
    dots_out[...] = jnp.where(lane == 0, part_dot, 0.0).astype(bf16)


def row_grads(grads, dots, own, oth, back):
    gate_grad, up_grad = grads[:, 0:HID], grads[:, HID : 2 * HID]
    counts = jnp.zeros((8, HID), f32)
    for k in range(8):
        counts = counts + own[k, 3 * BLK : SHARD, :].astype(f32)
        counts = counts + oth[k, 3 * BLK : SHARD, :].astype(f32)
    tally = jnp.sum(counts, axis=0, keepdims=True)[:, 0:BLK]
    px = []
    for ref in (own, oth):
        v = dot(gate_grad, weight(ref, 0), LAST) + dot(up_grad, weight(ref, 1), LAST)
        px.append(v.astype(bf16))
    to, fr = iota((256, 96), 0), iota((256, 96), 1)
    row = to & 7
    base = fr - 24 * ((to >> 3) & 3) - (to >> 5)
    paired = (row < 6) & (base == 8 * (row >> 1))
    first = one_hot(paired & ((row & 1) == 0))
    second = one_hot(paired & ((row & 1) == 1))
    c60 = one_hot((row == 6) & (base == 0))
    c61 = one_hot((row == 6) & (base == 8))
    c71 = one_hot((row == 7) & (base == 8))
    c72 = one_hot((row == 7) & (base == 16))
    for_dot = one_hot((row < CAP) & (base == 8 * row))
    count_at = (iota((256, BLK), 0) & 7) == CAP
    for j in range(2):

        def piece(k):
            v = px[k // 4]
            k = k % 4
            return v[96 * j : 96 * j + 96, 256 * k : 256 * k + 256]

        def store(v, lo, hi):
            for z in range(NZ):
                at = 64 * z + 32 * j
                back[at : at + 32, lo:hi] = v[32 * z : 32 * z + 32]

        lo, hi = piece(6), piece(7)
        ends = ((c60, lo, c71, hi), (c60, hi, c72, lo), (c61, lo, c72, hi))
        for n in range(3):
            a, va, b, vb = ends[n]
            v = dot(first, piece(n)) + dot(second, piece(n + 3)) + dot(a, va) + dot(b, vb)
            store(v.astype(bf16), 256 * n, 256 * n + 256)
        last = dot(for_dot, dots[96 * j : 96 * j + 96, :]) + jnp.where(count_at, tally, 0.0)
        store(last.astype(bf16), 768, BACK)


def weight_grads(x_rows, g_rows, grads, keep, send):
    half = DM // 2
    for ref, at in ((send, half), (keep, 0)):
        for k, rows in ((0, x_rows), (1, x_rows), (2, g_rows)):
            v = dot(rows[:, at : at + half], grads[:, k * HID : (k + 1) * HID], FIRST)
            ref[:, k * BLK : (k + 1) * BLK, :] = v.astype(bf16).reshape(8, BLK, HID)


def add_cores(keep, came, s0, s2, s4, s6, right, left):
    chip = lax.axis_index("x")

    def total(k):
        at = lax.rem(chip + k, 8)
        return (keep[at].astype(f32) + came[at].astype(f32)).astype(bf16)

    right[0 : 3 * BLK] = total(3)
    right[3 * BLK :] = total(1)
    s4[...] = total(4)
    left[0 : 3 * BLK] = total(5)
    left[3 * BLK :] = total(7)
    s2[...] = total(2)
    s6[...] = total(6)
    s0[...] = total(0)


def join_right(s2, right, s4, t2):
    near = right[0 : 3 * BLK].astype(f32)
    t2[...] = (s2[...].astype(f32) + near + s4[...].astype(f32)).astype(bf16)


def join_left(s6, left, t6):
    t6[...] = (s6[...].astype(f32) + left[0 : 3 * BLK].astype(f32)).astype(bf16)


def sum_chips(s0, right, left, t2, t6, gate, up, down):
    for k, ref in ((0, gate), (1, up), (2, down)):
        lo, hi = k * BLK, (k + 1) * BLK
        total = s0[lo:hi].astype(f32) + t2[lo:hi].astype(f32) + t6[lo:hi].astype(f32)
        lo, hi = lo + 3 * BLK, hi + 3 * BLK
        total = total + right[lo:hi].astype(f32) + left[lo:hi].astype(f32)
        ref[...] = (jnp.transpose(total) if k == 2 else total).astype(bf16)


def finish(back, routes, logits, grad_tokens, route_dot, aux_grad):
    core = lax.axis_index("c")
    _, _, member, slot = slots(routes[...])
    total = jnp.zeros((8, DM), f32)
    counts = jnp.zeros((1, BLK), f32)
    dots = []
    for x in range(2):
        s = jnp.zeros((8, BACK), f32)
        for n in range(32):
            at = 8 * (32 * x + n)
            s = s + back[at : at + 8, :].astype(f32)
        counts = counts + s[CAP : CAP + 1, 768:BACK]
        at = slot[:, x : x + 1].astype(i32)
        ends = (
            s[6:7, 0:512],
            jnp.concatenate([s[6:7, 512:768], s[7:8, 0:256]], axis=1),
            s[7:8, 256:768],
        )
        dot_x = jnp.zeros((8, 1), f32)
        for r in range(CAP):
            sel = jnp.where(at == r, member[:, x : x + 1], 0.0)
            row = jnp.concatenate(
                [s[2 * r : 2 * r + 1, 0:768], s[2 * r + 1 : 2 * r + 2, 0:768], ends[r]], axis=1
            )
            total = total + sel * row
            dot_x = dot_x + sel * s[r : r + 1, 768:769]
        dots.append(dot_x)
    grad_tokens[...] = in_order(total, core).astype(bf16)
    row2 = iota((2, 8), 0)
    route_dot[...] = jnp.where(row2 == 0, line(dots[0]), line(dots[1]))
    lg = logits[...]
    e = jnp.exp(lg - jnp.max(lg, axis=1, keepdims=True))
    probs = e / jnp.sum(e, axis=1, keepdims=True)
    cnt = counts[:, 0:8]
    target = 8.0 * (cnt / jnp.sum(cnt, axis=1, keepdims=True))
    aux_grad[...] = probs * (target - jnp.sum(probs * target, axis=1, keepdims=True))


def shifted(value, by):
    return lax.ppermute(value, "x", [(i, (i + by) % NX) for i in range(NX)])


def exchange(value, axis):
    return lax.all_to_all(value, axis, split_axis=0, concat_axis=0, tiled=True)


def body(tokens, cotangent, routes, logits, w_gate, w_up, w_down):
    routes_t = routes.T
    shard = call(pack_weights, shape(SHARD, HID), 4, limit=60)(routes_t, w_gate, w_up, w_down)
    rows = call(send_rows, shape(NZ, 8, DM), 4, limit=60)(tokens, cotangent, routes_t, logits)
    rows = exchange(rows, "z")
    rows = call(repack, shape(NY, 48, DM), 1)(rows.reshape(8 * NZ, DM))
    came = exchange(rows, "y")
    p2 = shifted(shard, 2)
    m2 = shifted(shard, 6)
    p1 = shifted(shard, 1)
    p4 = shifted(p2, 2)
    p3 = shifted(p2, 1)
    m3 = shifted(m2, 7)
    m1 = shifted(shard, 7)
    own = call(
        stack_shards,
        shape(8, SHARD, HID),
        8,
        far=HELD,
        scratch=(pltpu.SemaphoreType.DMA((len(HELD),)),),
    )(
        shard, p1, p2, p3, p4, m3, m2, m1
    )
    oth = lax.ppermute(own, "c", SWAP)
    x_rows, g_rows = call(unpack, (shape(ROWS, DM), shape(ROWS, DM)), 1)(came.reshape(48 * NY, DM))
    grads, dots, oth = call(
        forward,
        (shape(ROWS, 3 * HID), shape(ROWS, BLK), shape(8, SHARD, HID)),
        4,
        far=(3,),
        scratch=(pltpu.SemaphoreType.DMA,),
    )(x_rows, g_rows, own, oth)
    keep, send = call(
        weight_grads, (shape(8, 3 * BLK, HID), shape(8, 3 * BLK, HID)), 3
    )(x_rows, g_rows, grads)
    other = lax.ppermute(send, "c", SWAP)
    back = call(row_grads, shape(8 * NSRC, BACK), 4)(grads, dots, own, oth)
    one, two = shape(3 * BLK, HID), shape(6 * BLK, HID)
    s0, s2, s4, s6, right, left = call(add_cores, (one, one, one, one, two, two), 2)(keep, other)
    s4 = shifted(s4, 2)
    left = shifted(left, 7)
    back = exchange(back.reshape(NSRC, 8, BACK), ("z", "y"))
    right = shifted(right, 1)
    t6 = call(join_left, one, 2)(s6, left)
    t6 = shifted(t6, 6)
    t2 = call(join_right, one, 3)(s2, right, s4)
    t2 = shifted(t2, 2)
    grad_gate, grad_up, grad_down = call(
        sum_chips, (shape(BLK, HID), shape(BLK, HID), shape(HID, BLK)), 5
    )(s0, right, left, t2, t6)
    grad_tokens, route_dot, aux_grad = call(
        finish, (shape(8, DM), shape(2, 8, dtype=f32), shape(8, 8, dtype=f32)), 3
    )(back.reshape(8 * NSRC, BACK), routes_t, logits)
    return (grad_tokens, route_dot.T, aux_grad, grad_gate, grad_up, grad_down)


def solution(mesh):
    split = Mesh(mesh.devices.reshape(NX, NC, NZ, NY), ALL)
    rows, cols, down = P(ALL, None), P(("x", "c"), ("z", "y")), P(("z", "y"), ("x", "c"))

    return jax.shard_map(
        body,
        mesh=split,
        in_specs=(rows, rows, rows, rows, cols, cols, down),
        out_specs=(rows, rows, rows, cols, cols, down),
        check_vma=False,
    )
```

```python
import jax
import jax.numpy as jnp
from jax import lax
from jax.experimental import pallas as pl
from jax.experimental.pallas import tpu as pltpu
from jax.sharding import Mesh
from jax.sharding import PartitionSpec as P


NX, NC, NZ, NY = 8, 2, 8, 8
ALL = ("x", "c", "z", "y")
SWAP = ((0, 1), (1, 0))
CAP = 3
DM = 2048
HID = 256
BLK = 128
NSRC = NZ * NY
WIRE = 1536
BACK = 896
SHARD = 3 * BLK + 8
ROWS = NSRC * CAP
VM = pl.BlockSpec(memory_space=pltpu.VMEM)
FAR = pl.BlockSpec(memory_space=pltpu.HBM)
bf16, f32, i32 = jnp.bfloat16, jnp.float32, jnp.int32
FIRST = (((0,), (0,)), ((), ()))
LAST = (((1,), (1,)), ((), ()))


def dot(a, b, dims=(((1,), (0,)), ((), ()))):
    return lax.dot_general(a, b, dims, preferred_element_type=f32)


def call(kernel, outs, n_in, limit=16, far=(), scratch=()):
    specs = [FAR if k in far else VM for k in range(n_in)]
    return pl.pallas_call(
        kernel,
        out_shape=outs,
        in_specs=specs,
        out_specs=jax.tree.map(lambda _: VM, outs),
        scratch_shapes=scratch,
        compiler_params=pltpu.CompilerParams(vmem_limit_bytes=limit << 20),
    )


def shape(*dims, dtype=bf16):
    return jax.ShapeDtypeStruct(dims, dtype)


def iota(dims, axis):
    return lax.broadcasted_iota(i32, dims, axis)


def column(row):
    same = iota((8, 8), 0) == iota((8, 8), 1)
    return jnp.sum(jnp.where(same, row.astype(f32), 0.0), axis=1, keepdims=True)


def line(col):
    same = iota((8, 8), 0) == iota((8, 8), 1)
    return jnp.sum(jnp.where(same, col, 0.0), axis=0, keepdims=True)


def slots(routes_t):
    lane = iota((8, 8), 1).astype(f32)
    routes = (column(routes_t[0:1]), column(routes_t[1:2]))
    pick0 = (routes[0] == lane).astype(f32)
    pick1 = (routes[1] == lane).astype(f32)
    member = pick0 + pick1
    below = (iota((8, 8), 1) < iota((8, 8), 0)).astype(f32)
    slot = dot(below, member)
    return pick0, pick1, member, slot


def own_first(v, core):
    even = [v[:, 256 * k : 256 * k + 128] for k in range(8)]
    odd = [v[:, 256 * k + 128 : 256 * k + 256] for k in range(8)]
    mine = [jnp.where(core == 0, a, b) for a, b in zip(even, odd)]
    rest = [jnp.where(core == 0, b, a) for a, b in zip(even, odd)]
    return jnp.concatenate(mine + rest, axis=1)


def in_order(v, core):
    mine = [v[:, 128 * k : 128 * k + 128] for k in range(8)]
    rest = [v[:, 1024 + 128 * k : 1152 + 128 * k] for k in range(8)]
    both = []
    for a, b in zip(mine, rest):
        both += [jnp.where(core == 0, a, b), jnp.where(core == 0, b, a)]
    return jnp.concatenate(both, axis=1)


def pack_weights(routes, w_gate, w_up, w_down, out):
    out[0:BLK] = w_gate[...]
    out[BLK : 2 * BLK] = w_up[...]
    out[2 * BLK : 3 * BLK] = jnp.transpose(w_down[...].astype(f32)).astype(bf16)
    lane = iota((8, HID), 1).astype(f32)
    hits = (column(routes[0:1]) == lane).astype(f32) + (column(routes[1:2]) == lane).astype(f32)
    total = jnp.sum(hits, axis=0, keepdims=True)
    row = iota((8, HID), 0)
    out[3 * BLK : SHARD] = jnp.where(row == 0, total, 0.0).astype(bf16)


def send_rows(tokens, cotangent, routes, logits, out):
    core = lax.axis_index("c")
    pick0, pick1, member, slot = slots(routes[...])
    lg = logits[...]
    l0 = jnp.sum(pick0 * lg, axis=1, keepdims=True)
    l1 = jnp.sum(pick1 * lg, axis=1, keepdims=True)
    top = jnp.maximum(l0, l1)
    e0, e1 = jnp.exp(l0 - top), jnp.exp(l1 - top)
    both = e0 + e1
    scaled = pick0 * (e0 / both) + pick1 * (e1 / both)
    tok = own_first(tokens[...].astype(f32), core)
    cot = own_first(cotangent[...].astype(f32), core)
    lane = iota((8, 8), 1)
    tok_b = tok.astype(bf16)
    for x in range(2):
        mem, at = member[:, x : x + 1], slot[:, x : x + 1].astype(i32)
        sel_x = jnp.where((at == lane) & (lane < CAP), mem, 0.0).astype(bf16)
        sel_g = jnp.where((at + CAP == lane) & (lane < 2 * CAP), mem, 0.0).astype(bf16)
        grads = (cot * scaled[:, x : x + 1]).astype(bf16)
        rows = dot(sel_x, tok_b, FIRST) + dot(sel_g, grads, FIRST)
        tail = rows[:, WIRE:].astype(bf16)
        pieces = []
        for r in range(CAP):
            to, fr = iota((8, 8), 0), iota((8, 8), 1)
            move = ((to == 6) & (fr == r)) | ((to == 7) & (fr == CAP + r))
            moved = dot(move.astype(f32).astype(bf16), tail)
            pieces.append((rows[:, 512 * r : 512 * r + 512] + moved).astype(bf16))
        block = jnp.concatenate(pieces, axis=1)
        out[32 * x : 32 * x + 32] = jnp.broadcast_to(block[None], (32, 8, WIRE))


def stack_shards(*refs):
    out, chip = refs[8], lax.axis_index("x")
    for k in range(8):
        out[lax.rem(chip + 8 - k, 8)] = refs[k][...]


def one_hot(cond):
    return cond.astype(f32).astype(bf16)


def weight(ref, k):
    return ref[:, k * BLK : (k + 1) * BLK, :].reshape(DM // 2, HID)


def unpack(wire, x_out, g_out):
    to, fr = iota((192, 256), 0), iota((192, 256), 1)
    main = one_hot(fr == 8 * (to & 31) + (to >> 5))
    to, fr = iota((64, 256), 0), iota((64, 256), 1)
    ends = one_hot(fr == 8 * (to & 31) + 6 + (to >> 5))
    for j in range(2):
        part = dot(main, wire[256 * j : 256 * j + 256, :]).astype(bf16)
        x_out[96 * j : 96 * j + 96, 0:WIRE] = part[0:96]
        g_out[96 * j : 96 * j + 96, 0:WIRE] = part[96:192]
        for r in range(CAP):
            at = 96 * j + 32 * r
            tail = dot(ends, wire[256 * j : 256 * j + 256, 512 * r : 512 * r + 512]).astype(bf16)
            x_out[at : at + 32, WIRE:DM] = tail[0:32]
            g_out[at : at + 32, WIRE:DM] = tail[32:64]


def forward(x_rows, g_rows, own, far, grads_out, dots_out, oth, sem):
    fetch = pltpu.make_async_copy(far, oth, sem)
    fetch.start()
    half = DM // 2
    near = [dot(rows[:, 0:half], weight(own, k)) for k, rows in enumerate((x_rows, x_rows, g_rows))]
    fetch.wait()
    gate_pre, up_pre, hidden_grad = [
        near[k] + dot(rows[:, half:DM], weight(oth, k))
        for k, rows in enumerate((x_rows, x_rows, g_rows))
    ]
    sigma = 1.0 / (1.0 + jnp.exp(-gate_pre))
    active = gate_pre * sigma
    hidden = (active * up_pre).astype(bf16)
    part_dot = jnp.sum(hidden.astype(f32) * hidden_grad, axis=1, keepdims=True)
    up_grad = (hidden_grad * active).astype(bf16)
    gate_grad = (hidden_grad * up_pre * sigma * (1.0 + gate_pre * (1.0 - sigma))).astype(bf16)
    grads_out[:, 0:HID] = gate_grad
    grads_out[:, HID : 2 * HID] = up_grad
    grads_out[:, 2 * HID : 3 * HID] = hidden
    lane = iota((ROWS, BLK), 1)
    dots_out[...] = jnp.where(lane == 0, part_dot, 0.0).astype(bf16)


def row_grads(grads, dots, own, oth, back):
    gate_grad, up_grad = grads[:, 0:HID], grads[:, HID : 2 * HID]
    counts = jnp.zeros((8, HID), f32)
    for k in range(8):
        counts = counts + own[k, 3 * BLK : SHARD, :].astype(f32)
        counts = counts + oth[k, 3 * BLK : SHARD, :].astype(f32)
    tally = jnp.sum(counts, axis=0, keepdims=True)[:, 0:BLK]
    px = []
    for ref in (own, oth):
        v = dot(gate_grad, weight(ref, 0), LAST) + dot(up_grad, weight(ref, 1), LAST)
        px.append(v.astype(bf16))
    to, fr = iota((256, 96), 0), iota((256, 96), 1)
    row, slot_of = to & 7, fr >> 5
    same = (to >> 3) == (fr & 31)
    first = one_hot(same & (row == 2 * slot_of))
    second = one_hot(same & (row == 2 * slot_of + 1))
    c60 = one_hot(same & (row == 6) & (slot_of == 0))
    c61 = one_hot(same & (row == 6) & (slot_of == 1))
    c71 = one_hot(same & (row == 7) & (slot_of == 1))
    c72 = one_hot(same & (row == 7) & (slot_of == 2))
    for_dot = one_hot(same & (row == slot_of))
    count_at = (iota((256, BLK), 0) & 7) == CAP
    for j in range(2):

        def piece(k):
            v = px[k // 4]
            k = k % 4
            return v[96 * j : 96 * j + 96, 256 * k : 256 * k + 256]

        lo, hi = piece(6), piece(7)
        ends = ((c60, lo, c71, hi), (c60, hi, c72, lo), (c61, lo, c72, hi))
        for n in range(3):
            a, va, b, vb = ends[n]
            v = dot(first, piece(n)) + dot(second, piece(n + 3)) + dot(a, va) + dot(b, vb)
            back[256 * j : 256 * j + 256, 256 * n : 256 * n + 256] = v.astype(bf16)
        last = dot(for_dot, dots[96 * j : 96 * j + 96, :]) + jnp.where(count_at, tally, 0.0)
        back[256 * j : 256 * j + 256, 768:BACK] = last.astype(bf16)


def weight_grads(x_rows, g_rows, grads, keep, send):
    half = DM // 2
    for ref, at in ((send, half), (keep, 0)):
        for k, rows in ((0, x_rows), (1, x_rows), (2, g_rows)):
            v = dot(rows[:, at : at + half], grads[:, k * HID : (k + 1) * HID], FIRST)
            ref[:, k * BLK : (k + 1) * BLK, :] = v.astype(bf16).reshape(8, BLK, HID)


def add_cores(keep, came, s0, s2, s4, s6, right, left):
    chip = lax.axis_index("x")

    def total(k):
        at = lax.rem(chip + k, 8)
        return (keep[at].astype(f32) + came[at].astype(f32)).astype(bf16)

    right[0 : 3 * BLK] = total(3)
    right[3 * BLK :] = total(1)
    s4[...] = total(4)
    left[0 : 3 * BLK] = total(5)
    left[3 * BLK :] = total(7)
    s2[...] = total(2)
    s6[...] = total(6)
    s0[...] = total(0)


def join_right(s2, right, s4, t2):
    near = right[0 : 3 * BLK].astype(f32)
    t2[...] = (s2[...].astype(f32) + near + s4[...].astype(f32)).astype(bf16)


def join_left(s6, left, t6):
    t6[...] = (s6[...].astype(f32) + left[0 : 3 * BLK].astype(f32)).astype(bf16)


def sum_chips(s0, right, left, t2, t6, gate, up, down):
    for k, ref in ((0, gate), (1, up), (2, down)):
        lo, hi = k * BLK, (k + 1) * BLK
        total = s0[lo:hi].astype(f32) + t2[lo:hi].astype(f32) + t6[lo:hi].astype(f32)
        lo, hi = lo + 3 * BLK, hi + 3 * BLK
        total = total + right[lo:hi].astype(f32) + left[lo:hi].astype(f32)
        ref[...] = (jnp.transpose(total) if k == 2 else total).astype(bf16)


def finish(back, routes, logits, grad_tokens, route_dot, aux_grad):
    core = lax.axis_index("c")
    _, _, member, slot = slots(routes[...])
    total = jnp.zeros((8, DM), f32)
    counts = jnp.zeros((1, BLK), f32)
    dots = []
    for x in range(2):
        s = jnp.zeros((8, BACK), f32)
        for n in range(32):
            at = 8 * (32 * x + n)
            s = s + back[at : at + 8, :].astype(f32)
        counts = counts + s[CAP : CAP + 1, 768:BACK]
        at = slot[:, x : x + 1].astype(i32)
        ends = (
            s[6:7, 0:512],
            jnp.concatenate([s[6:7, 512:768], s[7:8, 0:256]], axis=1),
            s[7:8, 256:768],
        )
        dot_x = jnp.zeros((8, 1), f32)
        for r in range(CAP):
            sel = jnp.where(at == r, member[:, x : x + 1], 0.0)
            row = jnp.concatenate(
                [s[2 * r : 2 * r + 1, 0:768], s[2 * r + 1 : 2 * r + 2, 0:768], ends[r]], axis=1
            )
            total = total + sel * row
            dot_x = dot_x + sel * s[r : r + 1, 768:769]
        dots.append(dot_x)
    grad_tokens[...] = in_order(total, core).astype(bf16)
    row2 = iota((2, 8), 0)
    route_dot[...] = jnp.where(row2 == 0, line(dots[0]), line(dots[1]))
    lg = logits[...]
    e = jnp.exp(lg - jnp.max(lg, axis=1, keepdims=True))
    probs = e / jnp.sum(e, axis=1, keepdims=True)
    cnt = counts[:, 0:8]
    target = 8.0 * (cnt / jnp.sum(cnt, axis=1, keepdims=True))
    aux_grad[...] = probs * (target - jnp.sum(probs * target, axis=1, keepdims=True))


def shifted(value, by):
    return lax.ppermute(value, "x", [(i, (i + by) % NX) for i in range(NX)])


def exchange(value, axis):
    return lax.all_to_all(value, axis, split_axis=0, concat_axis=0, tiled=True)


def body(tokens, cotangent, routes, logits, w_gate, w_up, w_down):
    routes_t = routes.T
    shard = call(pack_weights, shape(SHARD, HID), 4)(routes_t, w_gate, w_up, w_down)
    p2 = shifted(shard, 2)
    m2 = shifted(shard, 6)
    wire = call(send_rows, shape(NSRC, 8, WIRE), 4, limit=60)(tokens, cotangent, routes_t, logits)
    came = exchange(wire, ("z", "y"))
    p1 = shifted(shard, 1)
    m1 = shifted(shard, 7)
    p4 = shifted(p2, 2)
    p3 = shifted(p2, 1)
    m3 = shifted(m2, 7)
    own = call(stack_shards, shape(8, SHARD, HID), 8)(shard, p1, p2, p3, p4, m3, m2, m1)
    oth = lax.ppermute(own, "c", SWAP)
    x_rows, g_rows = call(unpack, (shape(ROWS, DM), shape(ROWS, DM)), 1)(
        came.reshape(8 * NSRC, WIRE)
    )
    grads, dots, oth = call(
        forward,
        (shape(ROWS, 3 * HID), shape(ROWS, BLK), shape(8, SHARD, HID)),
        4,
        far=(3,),
        scratch=(pltpu.SemaphoreType.DMA,),
    )(x_rows, g_rows, own, oth)
    keep, send = call(
        weight_grads, (shape(8, 3 * BLK, HID), shape(8, 3 * BLK, HID)), 3
    )(x_rows, g_rows, grads)
    other = lax.ppermute(send, "c", SWAP)
    back = call(row_grads, shape(8 * NSRC, BACK), 4)(grads, dots, own, oth)
    one, two = shape(3 * BLK, HID), shape(6 * BLK, HID)
    s0, s2, s4, s6, right, left = call(add_cores, (one, one, one, one, two, two), 2)(keep, other)
    s4 = shifted(s4, 2)
    left = shifted(left, 7)
    back = exchange(back.reshape(NSRC, 8, BACK), ("z", "y"))
    right = shifted(right, 1)
    t6 = call(join_left, one, 2)(s6, left)
    t6 = shifted(t6, 6)
    t2 = call(join_right, one, 3)(s2, right, s4)
    t2 = shifted(t2, 2)
    grad_gate, grad_up, grad_down = call(
        sum_chips, (shape(BLK, HID), shape(BLK, HID), shape(HID, BLK)), 5
    )(s0, right, left, t2, t6)
    grad_tokens, route_dot, aux_grad = call(
        finish, (shape(8, DM), shape(2, 8, dtype=f32), shape(8, 8, dtype=f32)), 3
    )(back.reshape(8 * NSRC, BACK), routes_t, logits)
    return (grad_tokens, route_dot.T, aux_grad, grad_gate, grad_up, grad_down)


def solution(mesh):
    split = Mesh(mesh.devices.reshape(NX, NC, NZ, NY), ALL)
    rows, cols, down = P(ALL, None), P(("x", "c"), ("z", "y")), P(("z", "y"), ("x", "c"))

    return jax.shard_map(
        body,
        mesh=split,
        in_specs=(rows, rows, rows, rows, cols, cols, down),
        out_specs=(rows, rows, rows, cols, cols, down),
        check_vma=False,
    )
```

```python
import jax
import jax.numpy as jnp
from jax import lax
from jax.experimental import pallas as pl
from jax.experimental.pallas import tpu as pltpu
from jax.sharding import Mesh
from jax.sharding import PartitionSpec as P


NX, NC, NZ, NY = 8, 2, 8, 8
ALL = ("x", "c", "z", "y")
SWAP = ((0, 1), (1, 0))
CAP = 3
DM = 2048
HID = 256
BLK = 128
NSRC = NZ * NY
WIRE = 1536
BACK = 896
SHARD = 3 * BLK + 8
ROWS = NSRC * CAP
VM = pl.BlockSpec(memory_space=pltpu.VMEM)
FAR = pl.BlockSpec(memory_space=pltpu.HBM)
bf16, f32, i32 = jnp.bfloat16, jnp.float32, jnp.int32
FIRST = (((0,), (0,)), ((), ()))
LAST = (((1,), (1,)), ((), ()))


def dot(a, b, dims=(((1,), (0,)), ((), ()))):
    return lax.dot_general(a, b, dims, preferred_element_type=f32)


def call(kernel, outs, n_in, limit=16, far=(), scratch=()):
    specs = [FAR if k in far else VM for k in range(n_in)]
    return pl.pallas_call(
        kernel,
        out_shape=outs,
        in_specs=specs,
        out_specs=jax.tree.map(lambda _: VM, outs),
        scratch_shapes=scratch,
        compiler_params=pltpu.CompilerParams(vmem_limit_bytes=limit << 20),
    )


def shape(*dims, dtype=bf16):
    return jax.ShapeDtypeStruct(dims, dtype)


def iota(dims, axis):
    return lax.broadcasted_iota(i32, dims, axis)


def column(row):
    same = iota((8, 8), 0) == iota((8, 8), 1)
    return jnp.sum(jnp.where(same, row.astype(f32), 0.0), axis=1, keepdims=True)


def line(col):
    same = iota((8, 8), 0) == iota((8, 8), 1)
    return jnp.sum(jnp.where(same, col, 0.0), axis=0, keepdims=True)


def slots(routes_t):
    lane = iota((8, 8), 1).astype(f32)
    routes = (column(routes_t[0:1]), column(routes_t[1:2]))
    pick0 = (routes[0] == lane).astype(f32)
    pick1 = (routes[1] == lane).astype(f32)
    member = pick0 + pick1
    below = (iota((8, 8), 1) < iota((8, 8), 0)).astype(f32)
    slot = dot(below, member)
    return pick0, pick1, member, slot


def own_first(v, core):
    even = [v[:, 256 * k : 256 * k + 128] for k in range(8)]
    odd = [v[:, 256 * k + 128 : 256 * k + 256] for k in range(8)]
    mine = [jnp.where(core == 0, a, b) for a, b in zip(even, odd)]
    rest = [jnp.where(core == 0, b, a) for a, b in zip(even, odd)]
    return jnp.concatenate(mine + rest, axis=1)


def in_order(v, core):
    mine = [v[:, 128 * k : 128 * k + 128] for k in range(8)]
    rest = [v[:, 1024 + 128 * k : 1152 + 128 * k] for k in range(8)]
    both = []
    for a, b in zip(mine, rest):
        both += [jnp.where(core == 0, a, b), jnp.where(core == 0, b, a)]
    return jnp.concatenate(both, axis=1)


def pack_weights(routes, w_gate, w_up, w_down, out):
    out[0:BLK] = w_gate[...]
    out[BLK : 2 * BLK] = w_up[...]
    out[2 * BLK : 3 * BLK] = jnp.transpose(w_down[...].astype(f32)).astype(bf16)
    lane = iota((8, HID), 1).astype(f32)
    hits = (column(routes[0:1]) == lane).astype(f32) + (column(routes[1:2]) == lane).astype(f32)
    total = jnp.sum(hits, axis=0, keepdims=True)
    row = iota((8, HID), 0)
    out[3 * BLK : SHARD] = jnp.where(row == 0, total, 0.0).astype(bf16)


def send_rows(tokens, cotangent, routes, logits, out):
    core = lax.axis_index("c")
    pick0, pick1, member, slot = slots(routes[...])
    lg = logits[...]
    l0 = jnp.sum(pick0 * lg, axis=1, keepdims=True)
    l1 = jnp.sum(pick1 * lg, axis=1, keepdims=True)
    top = jnp.maximum(l0, l1)
    e0, e1 = jnp.exp(l0 - top), jnp.exp(l1 - top)
    both = e0 + e1
    scaled = pick0 * (e0 / both) + pick1 * (e1 / both)
    tok = own_first(tokens[...].astype(f32), core)
    cot = own_first(cotangent[...].astype(f32), core)
    lane = iota((8, 8), 1)
    tok_b = tok.astype(bf16)
    for x in range(2):
        mem, at = member[:, x : x + 1], slot[:, x : x + 1].astype(i32)
        sel_x = jnp.where((at == lane) & (lane < CAP), mem, 0.0).astype(bf16)
        sel_g = jnp.where((at + CAP == lane) & (lane < 2 * CAP), mem, 0.0).astype(bf16)
        grads = (cot * scaled[:, x : x + 1]).astype(bf16)
        rows = dot(sel_x, tok_b, FIRST) + dot(sel_g, grads, FIRST)
        tail = rows[:, WIRE:].astype(bf16)
        pieces = []
        for r in range(CAP):
            to, fr = iota((8, 8), 0), iota((8, 8), 1)
            move = ((to == 6) & (fr == r)) | ((to == 7) & (fr == CAP + r))
            moved = dot(move.astype(f32).astype(bf16), tail)
            pieces.append((rows[:, 512 * r : 512 * r + 512] + moved).astype(bf16))
        block = jnp.concatenate(pieces, axis=1)
        out[32 * x : 32 * x + 32] = jnp.broadcast_to(block[None], (32, 8, WIRE))


def stack_shards(*refs):
    out, chip = refs[8], lax.axis_index("x")
    for k in range(8):
        out[lax.rem(chip + 8 - k, 8)] = refs[k][...]


def one_hot(cond):
    return cond.astype(f32).astype(bf16)


def weight(ref, k):
    return ref[:, k * BLK : (k + 1) * BLK, :].reshape(DM // 2, HID)


def unpack(wire, x_out, g_out):
    to, fr = iota((192, 256), 0), iota((192, 256), 1)
    main = one_hot(fr == 8 * (to & 31) + (to >> 5))
    to, fr = iota((64, 256), 0), iota((64, 256), 1)
    ends = one_hot(fr == 8 * (to & 31) + 6 + (to >> 5))
    for j in range(2):
        part = dot(main, wire[256 * j : 256 * j + 256, :]).astype(bf16)
        x_out[96 * j : 96 * j + 96, 0:WIRE] = part[0:96]
        g_out[96 * j : 96 * j + 96, 0:WIRE] = part[96:192]
        for r in range(CAP):
            at = 96 * j + 32 * r
            tail = dot(ends, wire[256 * j : 256 * j + 256, 512 * r : 512 * r + 512]).astype(bf16)
            x_out[at : at + 32, WIRE:DM] = tail[0:32]
            g_out[at : at + 32, WIRE:DM] = tail[32:64]


def forward(x_rows, g_rows, own, far, grads_out, dots_out, oth, sem):
    fetch = pltpu.make_async_copy(far, oth, sem)
    fetch.start()
    half = DM // 2
    near = [dot(rows[:, 0:half], weight(own, k)) for k, rows in enumerate((x_rows, x_rows, g_rows))]
    fetch.wait()
    gate_pre, up_pre, hidden_grad = [
        near[k] + dot(rows[:, half:DM], weight(oth, k))
        for k, rows in enumerate((x_rows, x_rows, g_rows))
    ]
    sigma = 1.0 / (1.0 + jnp.exp(-gate_pre))
    active = gate_pre * sigma
    hidden = (active * up_pre).astype(bf16)
    part_dot = jnp.sum(hidden.astype(f32) * hidden_grad, axis=1, keepdims=True)
    up_grad = (hidden_grad * active).astype(bf16)
    gate_grad = (hidden_grad * up_pre * sigma * (1.0 + gate_pre * (1.0 - sigma))).astype(bf16)
    grads_out[:, 0:HID] = gate_grad
    grads_out[:, HID : 2 * HID] = up_grad
    grads_out[:, 2 * HID : 3 * HID] = hidden
    lane = iota((ROWS, BLK), 1)
    dots_out[...] = jnp.where(lane == 0, part_dot, 0.0).astype(bf16)


def row_grads(grads, dots, own, oth, back):
    gate_grad, up_grad = grads[:, 0:HID], grads[:, HID : 2 * HID]
    counts = jnp.zeros((8, HID), f32)
    for k in range(8):
        counts = counts + own[k, 3 * BLK : SHARD, :].astype(f32)
        counts = counts + oth[k, 3 * BLK : SHARD, :].astype(f32)
    tally = jnp.sum(counts, axis=0, keepdims=True)[:, 0:BLK]
    px = []
    for ref in (own, oth):
        v = dot(gate_grad, weight(ref, 0), LAST) + dot(up_grad, weight(ref, 1), LAST)
        px.append(v.astype(bf16))
    to, fr = iota((256, 96), 0), iota((256, 96), 1)
    row, slot_of = to & 7, fr >> 5
    same = (to >> 3) == (fr & 31)
    first = one_hot(same & (row == 2 * slot_of))
    second = one_hot(same & (row == 2 * slot_of + 1))
    c60 = one_hot(same & (row == 6) & (slot_of == 0))
    c61 = one_hot(same & (row == 6) & (slot_of == 1))
    c71 = one_hot(same & (row == 7) & (slot_of == 1))
    c72 = one_hot(same & (row == 7) & (slot_of == 2))
    for_dot = one_hot(same & (row == slot_of))
    count_at = (iota((256, BLK), 0) & 7) == CAP
    for j in range(2):

        def piece(k):
            v = px[k // 4]
            k = k % 4
            return v[96 * j : 96 * j + 96, 256 * k : 256 * k + 256]

        lo, hi = piece(6), piece(7)
        ends = ((c60, lo, c71, hi), (c60, hi, c72, lo), (c61, lo, c72, hi))
        for n in range(3):
            a, va, b, vb = ends[n]
            v = dot(first, piece(n)) + dot(second, piece(n + 3)) + dot(a, va) + dot(b, vb)
            back[256 * j : 256 * j + 256, 256 * n : 256 * n + 256] = v.astype(bf16)
        last = dot(for_dot, dots[96 * j : 96 * j + 96, :]) + jnp.where(count_at, tally, 0.0)
        back[256 * j : 256 * j + 256, 768:BACK] = last.astype(bf16)


def weight_grads(x_rows, g_rows, grads, keep, send):
    half = DM // 2
    for ref, at in ((send, half), (keep, 0)):
        for k, rows in ((0, x_rows), (1, x_rows), (2, g_rows)):
            v = dot(rows[:, at : at + half], grads[:, k * HID : (k + 1) * HID], FIRST)
            ref[:, k * BLK : (k + 1) * BLK, :] = v.astype(bf16).reshape(8, BLK, HID)


def add_cores(keep, came, *outs):
    chip = lax.axis_index("x")
    for k in range(8):
        at = lax.rem(chip + k, 8)
        outs[k][...] = (keep[at].astype(f32) + came[at].astype(f32)).astype(bf16)


def join_right(s2, right, s4, t2):
    total = s2[...].astype(f32) + right[...].astype(f32) + s4[...].astype(f32)
    t2[...] = total.astype(bf16)


def join_left(s6, left, t6):
    t6[...] = (s6[...].astype(f32) + left[...].astype(f32)).astype(bf16)


def sum_chips(s0, e1, e7, t2, t6, gate, up, down):
    for k, ref in ((0, gate), (1, up), (2, down)):
        lo, hi = k * BLK, (k + 1) * BLK
        total = s0[lo:hi].astype(f32) + t2[lo:hi].astype(f32) + t6[lo:hi].astype(f32)
        total = total + e1[lo:hi].astype(f32) + e7[lo:hi].astype(f32)
        ref[...] = (jnp.transpose(total) if k == 2 else total).astype(bf16)


def finish(back, routes, logits, grad_tokens, route_dot, aux_grad):
    core = lax.axis_index("c")
    _, _, member, slot = slots(routes[...])
    total = jnp.zeros((8, DM), f32)
    counts = jnp.zeros((1, BLK), f32)
    dots = []
    for x in range(2):
        s = jnp.zeros((8, BACK), f32)
        for n in range(32):
            at = 8 * (32 * x + n)
            s = s + back[at : at + 8, :].astype(f32)
        counts = counts + s[CAP : CAP + 1, 768:BACK]
        at = slot[:, x : x + 1].astype(i32)
        ends = (
            s[6:7, 0:512],
            jnp.concatenate([s[6:7, 512:768], s[7:8, 0:256]], axis=1),
            s[7:8, 256:768],
        )
        dot_x = jnp.zeros((8, 1), f32)
        for r in range(CAP):
            sel = jnp.where(at == r, member[:, x : x + 1], 0.0)
            row = jnp.concatenate(
                [s[2 * r : 2 * r + 1, 0:768], s[2 * r + 1 : 2 * r + 2, 0:768], ends[r]], axis=1
            )
            total = total + sel * row
            dot_x = dot_x + sel * s[r : r + 1, 768:769]
        dots.append(dot_x)
    grad_tokens[...] = in_order(total, core).astype(bf16)
    row2 = iota((2, 8), 0)
    route_dot[...] = jnp.where(row2 == 0, line(dots[0]), line(dots[1]))
    lg = logits[...]
    e = jnp.exp(lg - jnp.max(lg, axis=1, keepdims=True))
    probs = e / jnp.sum(e, axis=1, keepdims=True)
    cnt = counts[:, 0:8]
    target = 8.0 * (cnt / jnp.sum(cnt, axis=1, keepdims=True))
    aux_grad[...] = probs * (target - jnp.sum(probs * target, axis=1, keepdims=True))


def shifted(value, by):
    return lax.ppermute(value, "x", [(i, (i + by) % NX) for i in range(NX)])


def exchange(value, axis):
    return lax.all_to_all(value, axis, split_axis=0, concat_axis=0, tiled=True)


def body(tokens, cotangent, routes, logits, w_gate, w_up, w_down):
    routes_t = routes.T
    shard = call(pack_weights, shape(SHARD, HID), 4)(routes_t, w_gate, w_up, w_down)
    p2 = shifted(shard, 2)
    m2 = shifted(shard, 6)
    wire = call(send_rows, shape(NSRC, 8, WIRE), 4, limit=60)(tokens, cotangent, routes_t, logits)
    came = exchange(wire, ("z", "y"))
    p1 = shifted(shard, 1)
    m1 = shifted(shard, 7)
    p4 = shifted(p2, 2)
    p3 = shifted(p2, 1)
    m3 = shifted(m2, 7)
    own = call(stack_shards, shape(8, SHARD, HID), 8)(shard, p1, p2, p3, p4, m3, m2, m1)
    oth = lax.ppermute(own, "c", SWAP)
    x_rows, g_rows = call(unpack, (shape(ROWS, DM), shape(ROWS, DM)), 1)(
        came.reshape(8 * NSRC, WIRE)
    )
    grads, dots, oth = call(
        forward,
        (shape(ROWS, 3 * HID), shape(ROWS, BLK), shape(8, SHARD, HID)),
        4,
        far=(3,),
        scratch=(pltpu.SemaphoreType.DMA,),
    )(x_rows, g_rows, own, oth)
    keep, send = call(
        weight_grads, (shape(8, 3 * BLK, HID), shape(8, 3 * BLK, HID)), 3
    )(x_rows, g_rows, grads)
    other = lax.ppermute(send, "c", SWAP)
    back = call(row_grads, shape(8 * NSRC, BACK), 4)(grads, dots, own, oth)
    one = shape(3 * BLK, HID)
    s = call(add_cores, (one,) * 8, 2)(keep, other)
    far = shifted(s[4], 2)
    right = shifted(s[3], 1)
    back = exchange(back.reshape(NSRC, 8, BACK), ("z", "y"))
    left = shifted(s[5], 7)
    t2 = call(join_right, one, 3)(s[2], right, far)
    t2 = shifted(t2, 2)
    t6 = call(join_left, one, 2)(s[6], left)
    t6 = shifted(t6, 6)
    e1 = shifted(s[1], 1)
    e7 = shifted(s[7], 7)
    grad_gate, grad_up, grad_down = call(
        sum_chips, (shape(BLK, HID), shape(BLK, HID), shape(HID, BLK)), 5
    )(s[0], e1, e7, t2, t6)
    grad_tokens, route_dot, aux_grad = call(
        finish, (shape(8, DM), shape(2, 8, dtype=f32), shape(8, 8, dtype=f32)), 3
    )(back.reshape(8 * NSRC, BACK), routes_t, logits)
    return (grad_tokens, route_dot.T, aux_grad, grad_gate, grad_up, grad_down)


def solution(mesh):
    split = Mesh(mesh.devices.reshape(NX, NC, NZ, NY), ALL)
    rows, cols, down = P(ALL, None), P(("x", "c"), ("z", "y")), P(("z", "y"), ("x", "c"))

    return jax.shard_map(
        body,
        mesh=split,
        in_specs=(rows, rows, rows, rows, cols, cols, down),
        out_specs=(rows, rows, rows, cols, cols, down),
        check_vma=False,
    )
```
